64 devices in a mesh: req: 4 (over x, y), dap: 16 (over z, core).
Axes of the slice: x: 2, y: 2, z: 8, core: 2. Of those that a mesh axis runs over, the one named last changes fastest.
The devices are a block of a 4x4x8 slice.
Arguments:
- single: bfloat16 [1024, 384], P(('req', 'dap')), parts along dimension 0
- pair: bfloat16 [1024, 256, 128], P(('req', 'dap')), parts along dimension 0
- token_mask: int32 [1024], P(('req', 'dap')), parts along dimension 0
- tmo_proj: bfloat16 [2, 128, 512], replicated
- tmo_gate: bfloat16 [2, 128, 128], replicated
- tmo_out: bfloat16 [2, 128, 128], replicated
- tmi_proj: bfloat16 [2, 128, 512], replicated
- tmi_gate: bfloat16 [2, 128, 128], replicated
- tmi_out: bfloat16 [2, 128, 128], replicated
- tas_qkvg: bfloat16 [2, 128, 512], replicated
- tas_bias: bfloat16 [2, 128, 4], replicated
- tas_out: bfloat16 [2, 128, 128], replicated
- tae_qkvg: bfloat16 [2, 128, 512], replicated
- tae_bias: bfloat16 [2, 128, 4], replicated
- tae_out: bfloat16 [2, 128, 128], replicated
- pt_in: bfloat16 [2, 128, 1024], replicated
- pt_out: bfloat16 [2, 512, 128], replicated
- ap_qkvg: bfloat16 [2, 384, 1536], replicated
- ap_bias: bfloat16 [2, 128, 16], replicated
- ap_out: bfloat16 [2, 384, 384], replicated
- st_in: bfloat16 [2, 384, 3072], replicated
- st_out: bfloat16 [2, 1536, 384], replicated
Outputs:
- output 1: bfloat16 [1024, 384], P(('req', 'dap')), parts along dimension 0
- output 2: bfloat16 [1024, 256, 128], P(('req', 'dap')), parts along dimension 0
There are 4 independent parts. The reference program is written for one: setup_inputs(seed, part) draws one part's arguments, and reference() takes and returns one part's arrays. A program takes and returns all parts, laid end to end along the dimension named above; an argument that names none is the same for every part.
All inputs are finite; a program needn't handle non-finite values.
Results may differ from the reference program's by a relative error of at most 0.02.
Values are sent between devices in bfloat16 or wider.
A program may use at most 768 MiB of HBM per device.

```python
import jax
import jax.numpy as jnp
from jax import lax

TOKENS = 256
C_S = 384
C_Z = 128
TRI_HID = 128
TRI_HEADS = 4
TRI_DIM = 32
PAIR_FF = 512
S_HEADS = 16
S_DIM = 24
S_FF = 1536
BLOCKS = 2
EPS = 1e-5
NEG_BIG = 1e9


def weight_shapes():
    return [
        ('tmo_proj', (BLOCKS, C_Z, 4 * TRI_HID)),
        ('tmo_gate', (BLOCKS, C_Z, C_Z)),
        ('tmo_out', (BLOCKS, TRI_HID, C_Z)),
        ('tmi_proj', (BLOCKS, C_Z, 4 * TRI_HID)),
        ('tmi_gate', (BLOCKS, C_Z, C_Z)),
        ('tmi_out', (BLOCKS, TRI_HID, C_Z)),
        ('tas_qkvg', (BLOCKS, C_Z, 4 * TRI_HEADS * TRI_DIM)),
        ('tas_bias', (BLOCKS, C_Z, TRI_HEADS)),
        ('tas_out', (BLOCKS, TRI_HEADS * TRI_DIM, C_Z)),
        ('tae_qkvg', (BLOCKS, C_Z, 4 * TRI_HEADS * TRI_DIM)),
        ('tae_bias', (BLOCKS, C_Z, TRI_HEADS)),
        ('tae_out', (BLOCKS, TRI_HEADS * TRI_DIM, C_Z)),
        ('pt_in', (BLOCKS, C_Z, 2 * PAIR_FF)),
        ('pt_out', (BLOCKS, PAIR_FF, C_Z)),
        ('ap_qkvg', (BLOCKS, C_S, 4 * S_HEADS * S_DIM)),
        ('ap_bias', (BLOCKS, C_Z, S_HEADS)),
        ('ap_out', (BLOCKS, S_HEADS * S_DIM, C_S)),
        ('st_in', (BLOCKS, C_S, 2 * S_FF)),
        ('st_out', (BLOCKS, S_FF, C_S)),
    ]


def draw_weight(key, shape):
    return (jax.random.normal(key, shape, jnp.float32) * shape[-2] ** -0.5).astype(jnp.bfloat16)


def setup_inputs(seed: int = 0, part: int = 0) -> dict:
    part_key = jax.random.fold_in(jax.random.key(seed), part)
    key_single, key_pair, key_mask = jax.random.split(part_key, 3)
    shapes = weight_shapes()
    weight_keys = jax.random.split(jax.random.key(seed + 1), len(shapes))
    valid = jax.random.randint(key_mask, (), (3 * TOKENS) // 4, TOKENS + 1)
    inputs = {
        'single': jax.random.normal(key_single, (TOKENS, C_S), jnp.float32).astype(jnp.bfloat16),
        'pair': jax.random.normal(key_pair, (TOKENS, TOKENS, C_Z), jnp.float32).astype(jnp.bfloat16),
        'token_mask': (jnp.arange(TOKENS) < valid).astype(jnp.int32),
    }
    for index, (name, shape) in enumerate(shapes):
        inputs[name] = draw_weight(weight_keys[index], shape)
    return inputs


def linear(act_in, weight):
    flat = act_in.reshape(-1, act_in.shape[-1])
    out_flat = jnp.dot(flat, weight, preferred_element_type=jnp.float32)
    return out_flat.reshape(act_in.shape[:-1] + (weight.shape[-1],))


def layer_norm(values):
    values = values.astype(jnp.float32)
    centred = values - jnp.mean(values, axis=-1, keepdims=True)
    variance = jnp.mean(centred * centred, axis=-1, keepdims=True)
    return (centred * lax.rsqrt(variance + EPS)).astype(jnp.bfloat16)


def tri_mult(pair, mask_f, w_proj, w_gate, w_out, incoming):
    normed = layer_norm(pair)
    projected = linear(normed, w_proj)
    pair_mask = (mask_f[:, None] * mask_f[None, :])[:, :, None]
    left = (jax.nn.sigmoid(projected[..., TRI_HID:2 * TRI_HID]) * projected[..., :TRI_HID] * pair_mask).astype(jnp.bfloat16)
    right = (jax.nn.sigmoid(projected[..., 3 * TRI_HID:]) * projected[..., 2 * TRI_HID:3 * TRI_HID] * pair_mask).astype(jnp.bfloat16)
    form = 'kic,kjc->ijc' if incoming else 'ikc,jkc->ijc'
    product = jnp.einsum(form, left.astype(jnp.float32), right.astype(jnp.float32))
    gate = jax.nn.sigmoid(linear(normed, w_gate))
    update = linear(layer_norm(product), w_out)
    return (pair.astype(jnp.float32) + gate * update).astype(jnp.bfloat16)


def tri_att(pair, mask_f, w_qkvg, w_bias, w_out):
    normed = layer_norm(pair)
    bias = linear(normed, w_bias).astype(jnp.bfloat16).astype(jnp.float32)
    bias_hjk = jnp.moveaxis(bias, -1, 0)
    key_bias = (mask_f - 1.0) * NEG_BIG
    projected = linear(normed, w_qkvg).reshape(TOKENS, TOKENS, 4, TRI_HEADS, TRI_DIM)
    query_all = projected[:, :, 0].astype(jnp.bfloat16)
    key_all = projected[:, :, 1].astype(jnp.bfloat16)
    value_all = projected[:, :, 2].astype(jnp.bfloat16)
    gate = jax.nn.sigmoid(projected[:, :, 3])

    def one_row(row_in):
        q_row, k_row, v_row = row_in
        logits = jnp.einsum('jhd,khd->hjk', q_row.astype(jnp.float32), k_row.astype(jnp.float32)) * TRI_DIM ** -0.5 + bias_hjk + key_bias
        soft_scores = jax.nn.softmax(logits, axis=-1).astype(jnp.bfloat16)
        return jnp.einsum('hjk,khd->jhd', soft_scores.astype(jnp.float32), v_row.astype(jnp.float32))

    attended = lax.map(one_row, (query_all, key_all, value_all))
    merged = (attended * gate).astype(jnp.bfloat16).reshape(TOKENS, TOKENS, TRI_HEADS * TRI_DIM)
    return (pair.astype(jnp.float32) + linear(merged, w_out)).astype(jnp.bfloat16)


def transition(act_in, w_in, w_out):
    hidden = w_out.shape[0]
    projected = linear(layer_norm(act_in), w_in)
    inner = (jax.nn.silu(projected[..., :hidden]) * projected[..., hidden:]).astype(jnp.bfloat16)
    return (act_in.astype(jnp.float32) + linear(inner, w_out)).astype(jnp.bfloat16)


def single_att(single, pair, mask_f, w_qkvg, w_bias, w_out):
    projected = linear(layer_norm(single), w_qkvg).reshape(TOKENS, 4, S_HEADS, S_DIM)
    query_all = projected[:, 0].astype(jnp.bfloat16)
    key_all = projected[:, 1].astype(jnp.bfloat16)
    value_all = projected[:, 2].astype(jnp.bfloat16)
    gate = jax.nn.sigmoid(projected[:, 3])
    bias = jnp.einsum('ijc,ch->ihj', layer_norm(pair).astype(jnp.float32), w_bias.astype(jnp.float32)).astype(jnp.bfloat16).astype(jnp.float32)
    logits = jnp.einsum('ihd,jhd->ihj', query_all.astype(jnp.float32), key_all.astype(jnp.float32)) * S_DIM ** -0.5 + bias + (mask_f - 1.0) * NEG_BIG
    soft_scores = jax.nn.softmax(logits, axis=-1).astype(jnp.bfloat16)
    attended = jnp.einsum('ihj,jhd->ihd', soft_scores.astype(jnp.float32), value_all.astype(jnp.float32))
    merged = (attended * gate).astype(jnp.bfloat16).reshape(TOKENS, S_HEADS * S_DIM)
    return (single.astype(jnp.float32) + linear(merged, w_out)).astype(jnp.bfloat16)


def reference(single, pair, token_mask, tmo_proj, tmo_gate, tmo_out, tmi_proj, tmi_gate, tmi_out, tas_qkvg, tas_bias, tas_out, tae_qkvg, tae_bias, tae_out, pt_in, pt_out, ap_qkvg, ap_bias, ap_out, st_in, st_out):
    mask_f = token_mask.astype(jnp.float32)
    stacked = dict(tmo_proj=tmo_proj, tmo_gate=tmo_gate, tmo_out=tmo_out, tmi_proj=tmi_proj, tmi_gate=tmi_gate, tmi_out=tmi_out, tas_qkvg=tas_qkvg, tas_bias=tas_bias, tas_out=tas_out, tae_qkvg=tae_qkvg, tae_bias=tae_bias, tae_out=tae_out, pt_in=pt_in, pt_out=pt_out, ap_qkvg=ap_qkvg, ap_bias=ap_bias, ap_out=ap_out, st_in=st_in, st_out=st_out)

    def block(carry, layer):
        single_c, pair_c = carry
        pair_c = tri_mult(pair_c, mask_f, layer['tmo_proj'], layer['tmo_gate'], layer['tmo_out'], False)
        pair_c = tri_mult(pair_c, mask_f, layer['tmi_proj'], layer['tmi_gate'], layer['tmi_out'], True)
        pair_c = tri_att(pair_c, mask_f, layer['tas_qkvg'], layer['tas_bias'], layer['tas_out'])
        pair_c = jnp.swapaxes(tri_att(jnp.swapaxes(pair_c, 0, 1), mask_f, layer['tae_qkvg'], layer['tae_bias'], layer['tae_out']), 0, 1)
        pair_c = transition(pair_c, layer['pt_in'], layer['pt_out'])
        single_c = single_att(single_c, pair_c, mask_f, layer['ap_qkvg'], layer['ap_bias'], layer['ap_out'])
        single_c = transition(single_c, layer['st_in'], layer['st_out'])
        return (single_c, pair_c), None

    carry_out, stacked_none = lax.scan(block, (single, pair), stacked)
    single_out, pair_out = carry_out
    return single_out, pair_out
```

```python
import functools

import jax
import jax.numpy as jnp
from jax import lax
from jax.experimental import pallas as pl
from jax.experimental.pallas import tpu as pltpu
from jax.sharding import PartitionSpec as P

EPS = 1e-5
NEG_BIG = 1e9
LOG2E = 1.4426950408889634
F32 = jnp.float32
BF16 = jnp.bfloat16
MESH = pl.DeviceIdType.MESH
WEIGHT_NAMES = ('tmo_proj', 'tmo_gate', 'tmo_out', 'tmi_proj', 'tmi_gate', 'tmi_out', 'tas_qkvg', 'tas_bias', 'tas_out', 'tae_qkvg', 'tae_bias', 'tae_out', 'pt_in', 'pt_out', 'ap_qkvg', 'ap_bias', 'ap_out', 'st_in', 'st_out')
LANES = 128
VMEM_LIMIT = 60 * 1024 * 1024


def dot_nn(lhs, rhs):
    return lax.dot_general(lhs, rhs, (((1,), (0,)), ((), ())), preferred_element_type=F32)


def dot_nt(lhs, rhs):
    return lax.dot_general(lhs, rhs, (((1,), (1,)), ((), ())), preferred_element_type=F32)


def dot_tn(lhs, rhs):
    return lax.dot_general(lhs, rhs, (((0,), (0,)), ((), ())), preferred_element_type=F32)


def sigmoid(values):
    return 0.5 * jnp.tanh(0.5 * values) + 0.5


def layer_norm(values):
    values = values.astype(F32)
    centred = values - jnp.mean(values, axis=-1, keepdims=True)
    variance = jnp.mean(centred * centred, axis=-1, keepdims=True)
    return (centred * lax.rsqrt(variance + EPS)).astype(BF16)


def tri_mult_kernel(kind, layer, n_dev, z_hbm, mask_s, mask_v, w_proj, w_gate, w_out, *rest):
    if kind == 'colx':
        out_ref, zrow_ref = rest[:2]
        rest = rest[2:]
    else:
        out_ref, zrow_ref = rest[0], None
        rest = rest[1:]
    (zfull, b_full, a_full, z_t, stage, w_t, x_buf, x_in, in_sem, right_send, right_recv, left_send, left_recv, pair_send, pair_recv, x_send, x_recv) = rest
    chips = n_dev // 2
    rows = zfull.shape[2]
    half_c = b_full.shape[0]
    channels = 2 * half_c
    pad = half_c + 8
    me = lax.axis_index('dap')
    chip, core = me // 2, lax.rem(me, 2)
    partner = chip * 2 + 1 - core
    right = lax.rem(chip + 1, chips) * 2 + core
    left = lax.rem(chip + chips - 1, chips) * 2 + core

    loads = [pltpu.make_async_copy(z_hbm.at[:, pl.ds(h * LANES, LANES), :], zfull.at[me, h], in_sem.at[h]) for h in range(2)]
    for load in loads:
        load.start()
    barrier = pltpu.get_barrier_semaphore()
    for peer in (left, right, partner):
        pl.semaphore_signal(barrier, inc=1, device_id={'dap': peer}, device_id_type=MESH)
    w_t[...] = w_proj[layer].astype(F32).T.astype(BF16)
    for load in loads:
        load.wait()
    pl.semaphore_wait(barrier, 3)

    def send(block, half, send_sem, recv_sem, target):
        return pltpu.make_async_remote_copy(src_ref=zfull.at[block, half], dst_ref=zfull.at[block, half], send_sem=send_sem, recv_sem=recv_sem, device_id={'dap': target}, device_id_type=MESH)

    send(me, 0, right_send.at[0], right_recv.at[0], right).start()
    send(me, 1, left_send.at[0], left_recv.at[0], left).start()
    send(me, 1, right_send.at[1], right_recv.at[1], right).start()
    send(me, 0, left_send.at[1], left_recv.at[1], left).start()
    send(me, 0, pair_send.at[0], pair_recv.at[0], partner).start()
    send(me, 1, pair_send.at[1], pair_recv.at[1], partner).start()

    def weights(first):
        lo = pl.multiple_of(core * half_c, half_c)
        return jnp.concatenate([w_t[pl.ds(first * channels + lo, half_c), :], w_t[pl.ds((first + 1) * channels + lo, half_c), :]], axis=0)

    def project(load, row_mask, tok_mask, first, store):
        w_half = weights(first)

        @pl.loop(0, rows // 2)
        def _(pair):
            normed = layer_norm(load(pair))
            slab = dot_nt(w_half, normed)
            gated = sigmoid(slab[half_c:]) * slab[:half_c]
            for t in range(2):
                row = 2 * pair + t
                stage[pl.ds(pl.multiple_of(row * pad, 8), half_c), :] = gated[:, t * LANES:(t + 1) * LANES] * (tok_mask * row_mask(row))

        @pl.loop(0, half_c // 8)
        def _(group):
            for t in range(8):
                c = group * 8 + t
                store(c, stage[pl.ds(c, rows, stride=pad), :].astype(BF16))

    my_half = chip // (chips // 2)
    my_off = pl.multiple_of(lax.rem(chip, chips // 2) * 2 * rows, 2 * rows)

    def process(block, half):
        def load(pair):
            return zfull[block, half, pl.ds(2 * pair, 2)].reshape(2 * LANES, LANES)

        def store(c, values):
            b_full[c, half, pl.ds(pl.multiple_of(block * rows, rows), rows), :] = values

        project(load, lambda row: mask_s[block * rows + row], mask_v[half], 2, store)
        if kind != 'row':
            @pl.when(half == my_half)
            def _():
                @pl.loop(0, rows)
                def _(row):
                    stage[pl.ds(pl.multiple_of(row * pad, 8), 2 * rows), :] = zfull[block, half, row, pl.ds(my_off, 2 * rows), :].astype(F32)

                @pl.loop(0, rows // 4)
                def _(group):
                    for t in range(8):
                        i = group * 8 + t
                        z_t[i, pl.ds(pl.multiple_of(block * rows, rows), rows), :] = stage[pl.ds(i, rows, stride=pad), :].astype(BF16)

    def process_left_operand(who, half):
        spot = pl.multiple_of(who * rows, rows)

        def store(c, values):
            a_full[c, half, pl.ds(spot, rows), :] = values

        def load(pair):
            if kind == 'row':
                return zfull[chip * 2 + who, half, pl.ds(2 * pair, 2)].reshape(2 * LANES, LANES)
            return z_t[pl.ds(spot + 2 * pair, 2), pl.ds(pl.multiple_of(half * LANES, LANES), LANES), :].reshape(2 * LANES, LANES)

        project(load, lambda row: mask_s[(chip * 2 + who) * rows + row], mask_v[half], 0, store)

    @pl.loop(0, 4)
    def _(t):
        who, half = t // 2, lax.rem(t, 2)
        block = jnp.where(who == 0, me, partner)

        @pl.when(who == 1)
        def _():
            send(partner, half, pair_send.at[half], pair_recv.at[half], partner).wait_recv()

        process(block, half)

    if kind == 'row':
        @pl.loop(0, 4)
        def _(t):
            process_left_operand(t // 2, lax.rem(t, 2))

    events = chips - 1

    @pl.loop(0, events)
    def _(e):
        dist = e // 2 + 1
        half_r = lax.rem(e, 2)
        half_l = 1 - half_r
        from_left = lax.rem(chip - dist + chips, chips)
        from_right = lax.rem(chip + dist, chips)
        block_r, block_l = from_left * 2 + core, from_right * 2 + core
        send(block_r, half_r, right_send.at[e], right_recv.at[e], right).wait_recv()

        @pl.when(e + 2 < events)
        def _():
            send(block_r, half_r, right_send.at[e + 2], right_recv.at[e + 2], right).start()

        send(block_r, half_r, pair_send.at[2 * e + 2], pair_recv.at[2 * e + 2], partner).start()
        send(block_l, half_l, left_send.at[e], left_recv.at[e], left).wait_recv()

        @pl.when(e + 2 < events)
        def _():
            send(block_l, half_l, left_send.at[e + 2], left_recv.at[e + 2], left).start()

        send(block_l, half_l, pair_send.at[2 * e + 3], pair_recv.at[2 * e + 3], partner).start()

        @pl.loop(0, 4)
        def _(t):
            side, other = lax.rem(t, 2), t // 2
            owner = jnp.where(other == 0, core, 1 - core)
            block = jnp.where(side == 0, from_left, from_right) * 2 + owner
            half = jnp.where(side == 0, half_r, half_l)

            @pl.when(other == 1)
            def _():
                send(block, half, pair_send.at[2 * e + 2 + side], pair_recv.at[2 * e + 2 + side], partner).wait_recv()

            process(block, half)

    if kind != 'row':
        @pl.loop(0, 4)
        def _(t):
            process_left_operand(t // 2, lax.rem(t, 2))

    @pl.loop(0, half_c)
    def _(c):
        lhs = jnp.concatenate([a_full[c, 0], a_full[c, 1]], axis=1)
        rhs = jnp.concatenate([b_full[c, 0], b_full[c, 1]], axis=1)
        product = dot_nt(lhs, rhs) if kind == 'row' else dot_nn(lhs, rhs)
        for who in range(2):
            for half in range(2):
                x_buf[who, half, pl.ds(c, rows, stride=pad), :] = product[who * rows:(who + 1) * rows, half * LANES:(half + 1) * LANES]

    for e in range(events):
        send(me, 0, right_send.at[e], right_recv.at[e], right).wait_send()
        send(me, 0, left_send.at[e], left_recv.at[e], left).wait_send()
    for e in range(2 * events + 2):
        send(me, 0, pair_send.at[e], pair_recv.at[e], partner).wait_send()

    exchange = pltpu.make_async_remote_copy(src_ref=x_buf.at[1 - core], dst_ref=x_in, send_sem=x_send, recv_sem=x_recv, device_id={'dap': partner}, device_id_type=MESH)
    exchange.start()
    w_o = jnp.concatenate([w_out[layer, pl.ds(pl.multiple_of(core * half_c, half_c), half_c), :], w_out[layer, pl.ds(pl.multiple_of((1 - core) * half_c, half_c), half_c), :]], axis=0)
    exchange.wait()

    @pl.loop(0, rows)
    def _(i):
        for half in range(2):
            x = jnp.concatenate([x_buf[core, half, pl.ds(pl.multiple_of(i * pad, 8), half_c), :], x_in[half, pl.ds(pl.multiple_of(i * pad, 8), half_c), :]], axis=0)
            centred = x - jnp.mean(x, axis=0, keepdims=True)
            variance = jnp.mean(centred * centred, axis=0, keepdims=True)
            x_norm = (centred * lax.rsqrt(variance + EPS)).astype(BF16)
            update = dot_tn(x_norm, w_o)
            if kind == 'colx':
                z_row = z_t[core * rows + i, half * LANES:(half + 1) * LANES, :]
                zrow_ref[i, half * LANES:(half + 1) * LANES, :] = z_row
            else:
                z_row = zfull[me, half, i]
            gate = sigmoid(dot_nn(layer_norm(z_row), w_gate[layer]))
            out_ref[i, half * LANES:(half + 1) * LANES, :] = (z_row.astype(F32) + gate * update).astype(BF16)


def tri_mult(kind, layer, n_dev, cid, z, mask_s, mask_v, w_proj, w_gate, w_out):
    rows, tokens, channels = z.shape
    assert tokens == 2 * LANES and channels == LANES and rows * n_dev == tokens
    half_c = channels // 2
    pad = half_c + 8
    events = n_dev // 2 - 1
    vmem = pl.BlockSpec(memory_space=pltpu.VMEM)
    shape = jax.ShapeDtypeStruct(z.shape, BF16)
    dma = pltpu.SemaphoreType.DMA
    return pl.pallas_call(
        functools.partial(tri_mult_kernel, kind, layer, n_dev),
        out_shape=(shape, shape) if kind == 'colx' else shape,
        in_specs=[pl.BlockSpec(memory_space=pl.ANY), pl.BlockSpec(memory_space=pltpu.SMEM), vmem, vmem, vmem, vmem],
        out_specs=(vmem, vmem) if kind == 'colx' else vmem,
        scratch_shapes=[
            pltpu.VMEM((n_dev, 2, rows, LANES, channels), BF16),
            pltpu.VMEM((half_c, 2, tokens, LANES), BF16),
            pltpu.VMEM((half_c, 2, 2 * rows, LANES), BF16),
            pltpu.VMEM((2 * rows, tokens, channels), BF16),
            pltpu.VMEM((rows * pad, LANES), F32),
            pltpu.VMEM((4 * channels, channels), BF16),
            pltpu.VMEM((2, 2, rows * pad, LANES), F32),
            pltpu.VMEM((2, rows * pad, LANES), F32),
            dma((2,)), dma((events,)), dma((events,)), dma((events,)), dma((events,)), dma((2 * events + 2,)), dma((2 * events + 2,)), dma, dma,
        ],
        compiler_params=pltpu.CompilerParams(collective_id=cid, has_side_effects=True, vmem_limit_bytes=VMEM_LIMIT),
        name=f'tri_mult_{kind}_{cid}',
    )(z, mask_s, mask_v, w_proj, w_gate, w_out)


def tri_att_kernel(layer, n_dev, heads, turn, trans, z_ref, mask_c, w_qkvg, bias_t, w_out, *rest):
    if trans:
        pt_in, pt_out = rest[:2]
        rest = rest[2:]
    if turn:
        (out_ref, normed_s, bias_s, bias_all, logit_bias, w_t, k_s, q_s, v_s, g_s, z_new, r_buf, stage, b_send, b_recv, t_send, t_recv, own_sem) = rest
    else:
        (out_ref, normed_s, bias_s, bias_all, logit_bias, w_t, k_s, q_s, v_s, g_s, b_send, b_recv) = rest
        z_new = out_ref
    rows, tokens, channels = z_ref.shape
    width = channels // heads
    me = lax.axis_index('dap')
    barrier = pltpu.get_barrier_semaphore()
    peers = [lax.rem(me + p, n_dev) for p in range(1, n_dev)]
    for peer in peers:
        pl.semaphore_signal(barrier, inc=1, device_id={'dap': peer}, device_id_type=MESH)

    @pl.loop(0, rows)
    def _(i):
        normed = layer_norm(z_ref[i])
        normed_s[i] = normed
        slab = dot_nt(bias_t[layer], normed)
        for half in range(2):
            bias_s[half, pl.ds(pl.multiple_of(i * 8, 8), 8), :] = slab[:, half * LANES:(half + 1) * LANES]

    spot = pl.multiple_of(me * rows, rows)
    for h in range(heads):
        for half in range(2):
            bias_all[h, pl.ds(spot, rows), half * LANES:(half + 1) * LANES] = bias_s[half, pl.ds(h, rows, stride=8), :].astype(BF16)
    w_t[...] = w_qkvg[layer].astype(F32).T.astype(BF16)
    pl.semaphore_wait(barrier, n_dev - 1)

    def bias_copy(owner, p, target):
        ref = bias_all.at[:, pl.ds(pl.multiple_of(owner * rows, rows), rows), :]
        return pltpu.make_async_remote_copy(src_ref=ref, dst_ref=ref, send_sem=b_send.at[p - 1], recv_sem=b_recv.at[p - 1], device_id={'dap': target}, device_id_type=MESH)

    for p in range(1, n_dev):
        bias_copy(me, p, peers[p - 1]).start()

    @pl.loop(0, rows)
    def _(i):
        normed = normed_s[i]
        q_s[i] = dot_nt(w_t[:channels], normed).astype(BF16)
        k_s[i] = dot_nn(normed, w_qkvg[layer, :, channels:2 * channels]).astype(BF16)
        v_s[i] = dot_nt(w_t[2 * channels:3 * channels], normed).astype(BF16)
        g_s[i] = sigmoid(dot_nt(w_t[3 * channels:], normed))

    for p in range(1, n_dev):
        bias_copy(lax.rem(me + n_dev - p, n_dev), p, peers[p - 1]).wait_recv()
    for h in range(heads):
        for qh in range(2):
            for kh in range(2):
                tile = bias_all[h, qh * LANES:(qh + 1) * LANES, kh * LANES:(kh + 1) * LANES].astype(F32).T
                logit_bias[h, qh, kh * LANES:(kh + 1) * LANES, :] = (tile + mask_c[kh * LANES:(kh + 1) * LANES, :]) * LOG2E
    scale = width ** -0.5 * LOG2E

    def turn_copy(source, t, p, target, to):
        return pltpu.make_async_remote_copy(
            src_ref=z_new.at[pl.ds(4 * t, 4), pl.ds(pl.multiple_of(to * rows, rows), rows), :], dst_ref=r_buf.at[source, pl.ds(4 * t, 4)],
            send_sem=t_send.at[p - 1], recv_sem=t_recv.at[p - 1], device_id={'dap': target}, device_id_type=MESH)

    @pl.loop(0, rows)
    def _(i):
        keys = k_s[i]
        for qh in range(2):
            lanes = slice(qh * LANES, (qh + 1) * LANES)
            parts = []
            for h in range(heads):
                q_head = q_s[i, h * width:(h + 1) * width, lanes]
                pieces = [q_head]
                if h:
                    pieces = [jnp.zeros((h * width, LANES), BF16)] + pieces
                if h < heads - 1:
                    pieces = pieces + [jnp.zeros(((heads - 1 - h) * width, LANES), BF16)]
                logits = dot_nn(keys, jnp.concatenate(pieces, axis=0)) * scale + logit_bias[h, qh]
                weights = jnp.exp2(logits - jnp.max(logits, axis=0, keepdims=True))
                total = jnp.sum(weights, axis=0, keepdims=True)
                soft = (weights * (1.0 / total)).astype(BF16)
                parts.append(dot_nn(v_s[i, h * width:(h + 1) * width, :], soft))
            merged = (jnp.concatenate(parts, axis=0) * g_s[i, :, lanes]).astype(BF16)
            z_row = (z_ref[i, lanes, :].astype(F32) + dot_tn(merged, w_out[layer])).astype(BF16)
            if trans:
                normed = layer_norm(z_row)
                hidden = pt_out.shape[1]
                first = dot_nn(normed, pt_in[layer, :, :hidden])
                second = dot_nn(normed, pt_in[layer, :, hidden:])
                inner = (first * sigmoid(first) * second).astype(BF16)
                z_row = (z_row.astype(F32) + dot_nn(inner, pt_out[layer])).astype(BF16)
            z_new[i, lanes, :] = z_row
        if turn:
            @pl.when((lax.rem(i, 4) == 0) & (i > 0))
            def _():
                for p in range(1, n_dev):
                    turn_copy(me, i // 4 - 1, p, peers[p - 1], peers[p - 1]).start()

    if turn:
        own = pltpu.make_async_copy(z_new.at[:, pl.ds(spot, rows), :], r_buf.at[me], own_sem)
        own.start()
        for p in range(1, n_dev):
            turn_copy(me, rows // 4 - 1, p, peers[p - 1], peers[p - 1]).start()
        own.wait()

        def whole(source, p, target):
            return pltpu.make_async_remote_copy(src_ref=r_buf.at[source], dst_ref=r_buf.at[source], send_sem=t_send.at[p - 1], recv_sem=t_recv.at[p - 1], device_id={'dap': target}, device_id_type=MESH)

        def place(source):
            pad = rows + 8
            for i in range(rows):
                stage[i * pad:i * pad + rows, :] = r_buf[source, i].astype(F32)
            for j in range(rows):
                out_ref[j, pl.ds(pl.multiple_of(source * rows, rows), rows), :] = stage[pl.ds(j, rows, stride=pad), :].astype(BF16)

        place(me)

        @pl.loop(1, n_dev)
        def _(p):
            source = lax.rem(me + n_dev - p, n_dev)
            whole(source, p, lax.rem(me + p, n_dev)).wait_recv()
            place(source)

        for p in range(1, n_dev):
            whole(me, p, peers[p - 1]).wait_send()
    for p in range(1, n_dev):
        bias_copy(me, p, peers[p - 1]).wait_send()


def tri_att(layer, n_dev, cid, turn, z, mask_c, w_qkvg, bias_t, heads, w_out, pt=()):
    rows, tokens, channels = z.shape
    vmem = pl.BlockSpec(memory_space=pltpu.VMEM)
    dma = pltpu.SemaphoreType.DMA
    scratch = [
        pltpu.VMEM((rows, tokens, channels), BF16),
        pltpu.VMEM((2, rows * 8, LANES), F32),
        pltpu.VMEM((heads, tokens, tokens), BF16),
        pltpu.VMEM((heads, 2, tokens, LANES), F32),
        pltpu.VMEM((4 * channels, channels), BF16),
        pltpu.VMEM((rows, tokens, channels), BF16),
        pltpu.VMEM((rows, channels, tokens), BF16),
        pltpu.VMEM((rows, channels, tokens), BF16),
        pltpu.VMEM((rows, channels, tokens), F32),
    ]
    if turn:
        scratch += [pltpu.VMEM((rows, tokens, channels), BF16), pltpu.VMEM((n_dev, rows, rows, channels), BF16), pltpu.VMEM((rows * (rows + 8), LANES), F32)]
    scratch += [dma((n_dev - 1,)), dma((n_dev - 1,))]
    if turn:
        scratch += [dma((n_dev - 1,)), dma((n_dev - 1,)), dma]
    return pl.pallas_call(
        functools.partial(tri_att_kernel, layer, n_dev, heads, turn, bool(pt)),
        out_shape=jax.ShapeDtypeStruct(z.shape, BF16),
        in_specs=[vmem] * (5 + len(pt)),
        out_specs=vmem,
        scratch_shapes=scratch,
        compiler_params=pltpu.CompilerParams(collective_id=cid, has_side_effects=True, vmem_limit_bytes=VMEM_LIMIT),
        name=f'tri_att_{cid}',
    )(z, mask_c, w_qkvg, bias_t, w_out, *pt)


def transition(act_in, w_in, w_out):
    hidden = w_out.shape[0]
    projected = jnp.dot(layer_norm(act_in), w_in, preferred_element_type=F32)
    inner = (jax.nn.silu(projected[..., :hidden]) * projected[..., hidden:]).astype(BF16)
    return (act_in.astype(F32) + jnp.dot(inner, w_out, preferred_element_type=F32)).astype(BF16)


def single_step(single, pair, mask_all, w_qkvg, w_bias, w_out, st_in, st_out):
    rows = single.shape[0]
    heads = w_bias.shape[1]
    head_dim = w_qkvg.shape[1] // (4 * heads)
    projected = jnp.dot(layer_norm(single), w_qkvg, preferred_element_type=F32).reshape(rows, 4, heads, head_dim)
    query, gate = projected[:, 0].astype(BF16), jax.nn.sigmoid(projected[:, 3])
    kv_all = lax.all_gather(projected[:, 1:3].astype(BF16), 'dap', tiled=True)
    key_all, value_all = kv_all[:, 0], kv_all[:, 1]
    pair_bias = jnp.einsum('ijc,ch->ihj', layer_norm(pair), w_bias, preferred_element_type=F32).astype(BF16)
    logits = jnp.einsum('ihd,jhd->ihj', query, key_all, preferred_element_type=F32) * head_dim ** -0.5 + pair_bias.astype(F32) + (mask_all.astype(F32) - 1.0) * NEG_BIG
    soft_scores = jax.nn.softmax(logits, axis=-1).astype(BF16)
    attended = jnp.einsum('ihj,jhd->ihd', soft_scores, value_all, preferred_element_type=F32)
    merged = (attended * gate).astype(BF16).reshape(rows, -1)
    single = (single.astype(F32) + jnp.dot(merged, w_out, preferred_element_type=F32)).astype(BF16)
    return transition(single, st_in, st_out)


def solution(mesh):
    row_spec = P(('req', 'dap'))
    single_spec = P(('req', 'dap'), None)
    pair_spec = P(('req', 'dap'), None, None)
    n_dev = mesh.shape['dap']

    def local_program(single, pair, token_mask, *weights):
        w = dict(zip(WEIGHT_NAMES, weights))
        blocks = weights[0].shape[0]
        mask_all = lax.all_gather(token_mask, 'dap', tiled=True)
        tokens = mask_all.shape[0]
        mask_f = mask_all.astype(F32)
        mask_v = mask_f.reshape(2, 1, tokens // 2)
        mask_c = jnp.broadcast_to(((mask_f - 1.0) * NEG_BIG)[:, None], (tokens, LANES))
        heads = w['tas_bias'].shape[2]

        def bias_rows(name):
            turned = jnp.swapaxes(w[name], 1, 2)
            return jnp.pad(turned, ((0, 0), (0, 8 - heads), (0, 0)))

        tas_bias, tae_bias = bias_rows('tas_bias'), bias_rows('tae_bias')

        def single_block(b, single, pair_rows):
            return single_step(single, pair_rows, mask_all, *(w[name][b] for name in ('ap_qkvg', 'ap_bias', 'ap_out', 'st_in', 'st_out')))

        for b in range(blocks):
            cid = 4 * b
            out = (w['tmo_proj'], w['tmo_gate'], w['tmo_out'])
            if b == 0:
                pair = tri_mult('row', b, n_dev, cid, pair, mask_f, mask_v, *out)
            else:
                pair, pair_rows = tri_mult('colx', b, n_dev, cid, pair, mask_f, mask_v, *out)
                single = single_block(b - 1, single, pair_rows)
            pair = tri_mult('col', b, n_dev, cid + 1, pair, mask_f, mask_v, w['tmi_proj'], w['tmi_gate'], w['tmi_out'])
            pair = tri_att(b, n_dev, cid + 2, True, pair, mask_c, w['tas_qkvg'], tas_bias, heads, w['tas_out'])
            pair = tri_att(b, n_dev, cid + 3, b == blocks - 1, pair, mask_c, w['tae_qkvg'], tae_bias, heads, w['tae_out'], (w['pt_in'], w['pt_out']))
        single = single_block(blocks - 1, single, pair)
        return single, pair

    return jax.shard_map(local_program, mesh=mesh, in_specs=(single_spec, pair_spec, row_spec) + (P(),) * len(WEIGHT_NAMES), out_specs=(single_spec, pair_spec), check_vma=False)
```

```python
import functools

import jax
import jax.numpy as jnp
from jax import lax
from jax.experimental import pallas as pl
from jax.experimental.pallas import tpu as pltpu
from jax.sharding import PartitionSpec as P

EPS = 1e-5
NEG_BIG = 1e9
LOG2E = 1.4426950408889634
F32 = jnp.float32
BF16 = jnp.bfloat16
MESH = pl.DeviceIdType.MESH
WEIGHT_NAMES = ('tmo_proj', 'tmo_gate', 'tmo_out', 'tmi_proj', 'tmi_gate', 'tmi_out', 'tas_qkvg', 'tas_bias', 'tas_out', 'tae_qkvg', 'tae_bias', 'tae_out', 'pt_in', 'pt_out', 'ap_qkvg', 'ap_bias', 'ap_out', 'st_in', 'st_out')
LANES = 128
VMEM_LIMIT = 60 * 1024 * 1024


def dot_nn(lhs, rhs):
    return lax.dot_general(lhs, rhs, (((1,), (0,)), ((), ())), preferred_element_type=F32)


def turned(values):
    return values.astype(F32).T.astype(BF16)


def dot_nt(lhs, rhs):
    return lax.dot_general(lhs, rhs, (((1,), (1,)), ((), ())), preferred_element_type=F32)


def dot_tn(lhs, rhs):
    return lax.dot_general(lhs, rhs, (((0,), (0,)), ((), ())), preferred_element_type=F32)


def sigmoid(values):
    return 0.5 * jnp.tanh(0.5 * values) + 0.5


def layer_norm_t(values):
    values = values.astype(F32)
    centred = values - jnp.mean(values, axis=0, keepdims=True)
    variance = jnp.mean(centred * centred, axis=0, keepdims=True)
    return (centred * lax.rsqrt(variance + EPS)).astype(BF16)


def layer_norm(values):
    values = values.astype(F32)
    centred = values - jnp.mean(values, axis=-1, keepdims=True)
    variance = jnp.mean(centred * centred, axis=-1, keepdims=True)
    return (centred * lax.rsqrt(variance + EPS)).astype(BF16)


def tri_mult_kernel(kind, layer, n_dev, z_hbm, mask_s, mask_v, w_proj, w_gate, w_out, out_ref, *rest):
    if kind == 'row':
        (zfull, b_full, a_full, stage, w_t, x_buf, x_in, in_sem, right_send, right_recv, left_send, left_recv, pair_send, pair_recv, x_send, x_recv) = rest
    else:
        (zfull, b_full, a_full, a_turn, stage, w_t, x_buf, x_in, in_sem, right_send, right_recv, left_send, left_recv, pair_send, pair_recv, x_send, x_recv) = rest
    chips = n_dev // 2
    rows = zfull.shape[2]
    half_c = b_full.shape[0]
    channels = 2 * half_c
    pad = half_c + 8
    me = lax.axis_index('dap')
    chip, core = me // 2, lax.rem(me, 2)
    partner = chip * 2 + 1 - core
    right = lax.rem(chip + 1, chips) * 2 + core
    left = lax.rem(chip + chips - 1, chips) * 2 + core

    loads = [pltpu.make_async_copy(z_hbm.at[:, :, pl.ds(h * LANES, LANES)], zfull.at[me, h], in_sem.at[h]) for h in range(2)]
    for load in loads:
        load.start()
    barrier = pltpu.get_barrier_semaphore()
    for peer in (left, right, partner):
        pl.semaphore_signal(barrier, inc=1, device_id={'dap': peer}, device_id_type=MESH)
    for load in loads:
        load.wait()
    pl.semaphore_wait(barrier, 3)

    def send(block, half, send_sem, recv_sem, target):
        return pltpu.make_async_remote_copy(src_ref=zfull.at[block, half], dst_ref=zfull.at[block, half], send_sem=send_sem, recv_sem=recv_sem, device_id={'dap': target}, device_id_type=MESH)

    send(me, 0, right_send.at[0], right_recv.at[0], right).start()
    send(me, 1, left_send.at[0], left_recv.at[0], left).start()
    send(me, 1, right_send.at[1], right_recv.at[1], right).start()
    send(me, 0, left_send.at[1], left_recv.at[1], left).start()
    send(me, 0, pair_send.at[0], pair_recv.at[0], partner).start()
    send(me, 1, pair_send.at[1], pair_recv.at[1], partner).start()

    x_buf[0, 0, :4 * channels, :] = w_proj[layer].astype(F32).T
    for spot, part in enumerate((2, 3, 0, 1)):
        w_t[spot * half_c:(spot + 1) * half_c, :] = x_buf[0, 0, pl.ds(pl.multiple_of(part * channels + core * half_c, half_c), half_c), :].astype(BF16)

    my_half = chip // (chips // 2)
    my_off = pl.multiple_of(lax.rem(chip, chips // 2) * 2 * rows, 2 * rows)

    def project(block, half, operands):
        tok_mask = mask_v[half]
        weights = w_t[:operands * channels, :]

        @pl.loop(0, rows // 2)
        def _(pair):
            normed = jnp.concatenate([layer_norm_t(zfull[block, half, 2 * pair + t]) for t in range(2)], axis=1)
            slab = dot_nn(weights, normed)
            for o in range(operands):
                gated = sigmoid(slab[o * channels + half_c:(o + 1) * channels]) * slab[o * channels:o * channels + half_c]
                for t in range(2):
                    row = 2 * pair + t
                    stage[o, pl.ds(pl.multiple_of(row * pad, 8), half_c), :] = gated[:, t * LANES:(t + 1) * LANES] * (tok_mask * mask_s[block * rows + row])

        spot = pl.multiple_of(block * rows, rows)

        @pl.loop(0, half_c // 16)
        def _(group):
            for t in range(16):
                c = group * 16 + t
                b_full[c, half, pl.ds(spot, rows), :] = stage[0, pl.ds(c, rows, stride=pad), :].astype(BF16)
                if operands == 2:
                    left_operand = stage[1, pl.ds(c, rows, stride=pad), :].astype(BF16)
                    if kind == 'row':
                        a_full[c, half, pl.ds(pl.multiple_of(lax.rem(block, 2) * rows, rows), rows), :] = left_operand
                    else:
                        a_full[c, pl.ds(spot, rows), :] = left_operand

    def process(block, half, mine):
        if kind == 'row':
            project(block, half, 2 if mine else 1)
        else:
            @pl.when(half == my_half)
            def _():
                project(block, half, 2)

            @pl.when(half != my_half)
            def _():
                project(block, half, 1)

    @pl.loop(0, 4)
    def _(t):
        who, half = t // 2, lax.rem(t, 2)
        block = jnp.where(who == 0, me, partner)

        @pl.when(who == 1)
        def _():
            send(partner, half, pair_send.at[half], pair_recv.at[half], partner).wait_recv()

        process(block, half, True)

    events = chips - 1

    @pl.loop(0, events)
    def _(e):
        dist = e // 2 + 1
        half_r = lax.rem(e, 2)
        half_l = 1 - half_r
        from_left = lax.rem(chip - dist + chips, chips)
        from_right = lax.rem(chip + dist, chips)
        block_r, block_l = from_left * 2 + core, from_right * 2 + core
        send(block_r, half_r, right_send.at[e], right_recv.at[e], right).wait_recv()

        @pl.when(e + 2 < events)
        def _():
            send(block_r, half_r, right_send.at[e + 2], right_recv.at[e + 2], right).start()

        send(block_r, half_r, pair_send.at[2 * e + 2], pair_recv.at[2 * e + 2], partner).start()
        send(block_l, half_l, left_send.at[e], left_recv.at[e], left).wait_recv()

        @pl.when(e + 2 < events)
        def _():
            send(block_l, half_l, left_send.at[e + 2], left_recv.at[e + 2], left).start()

        send(block_l, half_l, pair_send.at[2 * e + 3], pair_recv.at[2 * e + 3], partner).start()

        @pl.loop(0, 4)
        def _(t):
            side, other = lax.rem(t, 2), t // 2
            owner = jnp.where(other == 0, core, 1 - core)
            block = jnp.where(side == 0, from_left, from_right) * 2 + owner
            half = jnp.where(side == 0, half_r, half_l)

            @pl.when(other == 1)
            def _():
                send(block, half, pair_send.at[2 * e + 2 + side], pair_recv.at[2 * e + 2 + side], partner).wait_recv()

            process(block, half, False)

    if kind != 'row':
        @pl.loop(0, half_c // 4)
        def _(group):
            for t in range(4):
                a_turn[group * 4 + t] = a_full[group * 4 + t].T

    @pl.loop(0, half_c // 4)
    def _(group):
        for t in range(4):
            c = group * 4 + t
            rhs = jnp.concatenate([b_full[c, 0], b_full[c, 1]], axis=1)
            if kind == 'row':
                product = dot_nt(jnp.concatenate([a_full[c, 0], a_full[c, 1]], axis=1), rhs)
            else:
                product = dot_nn(a_turn[c, pl.ds(my_off, 2 * rows), :], rhs)
            for who in range(2):
                for half in range(2):
                    x_buf[who, half, pl.ds(c, rows, stride=pad), :] = product[who * rows:(who + 1) * rows, half * LANES:(half + 1) * LANES]

    exchange = pltpu.make_async_remote_copy(src_ref=x_buf.at[1 - core], dst_ref=x_in, send_sem=x_send, recv_sem=x_recv, device_id={'dap': partner}, device_id_type=MESH)
    for e in range(events):
        send(me, 0, right_send.at[e], right_recv.at[e], right).wait_send()
        send(me, 0, left_send.at[e], left_recv.at[e], left).wait_send()
    for e in range(2 * events + 2):
        send(me, 0, pair_send.at[e], pair_recv.at[e], partner).wait_send()
    exchange.start()
    w_own = w_out[layer, pl.ds(pl.multiple_of(core * half_c, half_c), half_c), :]
    w_other = w_out[layer, pl.ds(pl.multiple_of((1 - core) * half_c, half_c), half_c), :]
    w_t[:channels, :] = turned(jnp.concatenate([w_own, w_other], axis=0))
    w_t[channels:2 * channels, :] = turned(w_gate[layer])
    exchange.wait()

    @pl.loop(0, rows)
    def _(i):
        for half in range(2):
            x = jnp.concatenate([x_buf[core, half, pl.ds(pl.multiple_of(i * pad, 8), half_c), :], x_in[half, pl.ds(pl.multiple_of(i * pad, 8), half_c), :]], axis=0)
            update = dot_nn(w_t[:channels, :], layer_norm_t(x))
            z_row = zfull[me, half, i]
            gate = sigmoid(dot_nn(w_t[channels:2 * channels, :], layer_norm_t(z_row)))
            out_ref[i, :, half * LANES:(half + 1) * LANES] = (z_row.astype(F32) + gate * update).astype(BF16)


def tri_mult(kind, layer, n_dev, cid, z, mask_s, mask_v, w_proj, w_gate, w_out):
    rows, channels, tokens = z.shape
    assert tokens == 2 * LANES and channels == LANES and rows * n_dev == tokens
    half_c = channels // 2
    pad = half_c + 8
    events = n_dev // 2 - 1
    vmem = pl.BlockSpec(memory_space=pltpu.VMEM)
    dma = pltpu.SemaphoreType.DMA
    left_operand = [pltpu.VMEM((half_c, 2, 2 * rows, LANES), BF16)]
    if kind != 'row':
        left_operand = [pltpu.VMEM((half_c, tokens, LANES), BF16), pltpu.VMEM((half_c, LANES, tokens), BF16)]
    return pl.pallas_call(
        functools.partial(tri_mult_kernel, kind, layer, n_dev),
        out_shape=jax.ShapeDtypeStruct(z.shape, BF16),
        in_specs=[pl.BlockSpec(memory_space=pl.ANY), pl.BlockSpec(memory_space=pltpu.SMEM), vmem, vmem, vmem, vmem],
        out_specs=vmem,
        scratch_shapes=[
            pltpu.VMEM((n_dev, 2, rows, channels, LANES), BF16),
            pltpu.VMEM((half_c, 2, tokens, LANES), BF16),
            *left_operand,
            pltpu.VMEM((2, rows * pad, LANES), F32),
            pltpu.VMEM((2 * channels, channels), BF16),
            pltpu.VMEM((2, 2, rows * pad, LANES), F32),
            pltpu.VMEM((2, rows * pad, LANES), F32),
            dma((2,)), dma((events,)), dma((events,)), dma((events,)), dma((events,)), dma((2 * events + 2,)), dma((2 * events + 2,)), dma, dma,
        ],
        compiler_params=pltpu.CompilerParams(collective_id=cid, has_side_effects=True, vmem_limit_bytes=VMEM_LIMIT),
        name=f'tri_mult_{kind}_{cid}',
    )(z, mask_s, mask_v, w_proj, w_gate, w_out)


def tri_att_kernel(layer, n_dev, heads, last, trans, share, z_ref, mask_c, w_qkvg, bias_t, w_out, *rest):
    rest = list(rest)
    pt_in, pt_out = (rest.pop(0), rest.pop(0)) if trans else (None, None)
    kv_in = rest.pop(0) if share else None
    out_ref = rest.pop(0)
    kv_all = rest.pop(0) if share else None
    (normed_s, bias_s, bias_all, logit_bias, w_t, w_o, k_s, q_s, v_s, g_s, z_nat, r_buf, stage, b_send, b_recv, t_send, t_recv, own_sem) = rest[:18]
    rest = rest[18:]
    pt_in_t, pt_out_t = (rest.pop(0), rest.pop(0)) if trans else (None, None)
    kv_buf, kv_send, kv_recv = (rest.pop(0), rest.pop(0), rest.pop(0)) if share else (None, None, None)
    rows, channels, tokens = z_ref.shape
    width = channels // heads
    me = lax.axis_index('dap')
    barrier = pltpu.get_barrier_semaphore()
    peers = [lax.rem(me + p, n_dev) for p in range(1, n_dev)]
    for peer in peers:
        pl.semaphore_signal(barrier, inc=1, device_id={'dap': peer}, device_id_type=MESH)

    @pl.loop(0, rows)
    def _(i):
        normed = layer_norm_t(z_ref[i])
        normed_s[i] = normed
        slab = dot_nn(bias_t[layer], normed)
        for half in range(2):
            bias_s[half, pl.ds(pl.multiple_of(i * 8, 8), 8), :] = slab[:, half * LANES:(half + 1) * LANES]

    spot = pl.multiple_of(me * rows, rows)
    for h in range(heads):
        for half in range(2):
            bias_all[h, pl.ds(spot, rows), half * LANES:(half + 1) * LANES] = bias_s[half, pl.ds(h, rows, stride=8), :].astype(BF16)
    if share:
        kv_buf[pl.ds(spot, rows), :] = kv_in[...]
    w_t[...] = turned(w_qkvg[layer])
    w_o[...] = turned(w_out[layer])
    if trans:
        for part in range(0, pt_in_t.shape[0], channels):
            pt_in_t[part:part + channels, :] = turned(pt_in[layer, :, part:part + channels])
        pt_out_t[...] = turned(pt_out[layer])
    pl.semaphore_wait(barrier, n_dev - 1)

    def bias_copy(owner, p, target):
        ref = bias_all.at[:, pl.ds(pl.multiple_of(owner * rows, rows), rows), :]
        return pltpu.make_async_remote_copy(src_ref=ref, dst_ref=ref, send_sem=b_send.at[p - 1], recv_sem=b_recv.at[p - 1], device_id={'dap': target}, device_id_type=MESH)

    def kv_copy(owner, p, target):
        ref = kv_buf.at[pl.ds(pl.multiple_of(owner * rows, rows), rows), :]
        return pltpu.make_async_remote_copy(src_ref=ref, dst_ref=ref, send_sem=kv_send.at[p - 1], recv_sem=kv_recv.at[p - 1], device_id={'dap': target}, device_id_type=MESH)

    for p in range(1, n_dev):
        bias_copy(me, p, peers[p - 1]).start()
    if share:
        for p in range(1, n_dev):
            kv_copy(me, p, peers[p - 1]).start()

    @pl.loop(0, rows)
    def _(i):
        slab = dot_nn(w_t[...], normed_s[i])
        q_s[i] = slab[:channels].astype(BF16)
        k_s[i] = slab[channels:2 * channels].T.astype(BF16)
        v_s[i] = slab[2 * channels:3 * channels].astype(BF16)
        g_s[i] = sigmoid(slab[3 * channels:])

    for p in range(1, n_dev):
        bias_copy(lax.rem(me + n_dev - p, n_dev), p, peers[p - 1]).wait_recv()
    for h in range(heads):
        for qh in range(2):
            for kh in range(2):
                tile = bias_all[h, qh * LANES:(qh + 1) * LANES, kh * LANES:(kh + 1) * LANES].astype(F32).T
                logit_bias[h, kh * LANES:(kh + 1) * LANES, qh * LANES:(qh + 1) * LANES] = (tile + mask_c[kh * LANES:(kh + 1) * LANES, :]) * LOG2E
    scale = width ** -0.5 * LOG2E

    def turn_copy(source, t, p, target, to):
        return pltpu.make_async_remote_copy(
            src_ref=z_nat.at[pl.ds(4 * t, 4), pl.ds(pl.multiple_of(to * rows, rows), rows), :], dst_ref=r_buf.at[source, pl.ds(4 * t, 4)],
            send_sem=t_send.at[p - 1], recv_sem=t_recv.at[p - 1], device_id={'dap': target}, device_id_type=MESH)

    @pl.loop(0, rows)
    def _(i):
        keys = k_s[i]
        parts = []
        for h in range(heads):
            pieces = [q_s[i, h * width:(h + 1) * width, :]]
            if h:
                pieces = [jnp.zeros((h * width, tokens), BF16)] + pieces
            if h < heads - 1:
                pieces = pieces + [jnp.zeros(((heads - 1 - h) * width, tokens), BF16)]
            scores = dot_nn(keys, jnp.concatenate(pieces, axis=0))
            halves = []
            for qh in range(2):
                lanes = slice(qh * LANES, (qh + 1) * LANES)
                logits = scores[:, lanes] * scale + logit_bias[h, :, lanes]
                weights = jnp.exp2(logits - jnp.max(logits, axis=0, keepdims=True))
                total = jnp.sum(weights, axis=0, keepdims=True)
                halves.append((weights * (1.0 / total)).astype(BF16))
            parts.append(dot_nn(v_s[i, h * width:(h + 1) * width, :], jnp.concatenate(halves, axis=1)))
        merged = (jnp.concatenate(parts, axis=0) * g_s[i]).astype(BF16)
        z_row = (z_ref[i].astype(F32) + dot_nn(w_o[...], merged)).astype(BF16)
        if trans:
            normed = layer_norm_t(z_row)
            hidden = pt_out.shape[1]
            update = jnp.zeros((channels, tokens), F32)
            for part in range(0, hidden, channels):
                first = dot_nn(pt_in_t[part:part + channels, :], normed)
                second = dot_nn(pt_in_t[hidden + part:hidden + part + channels, :], normed)
                update = update + dot_nn(pt_out_t[:, part:part + channels], (first * sigmoid(first) * second).astype(BF16))
            z_row = (z_row.astype(F32) + update).astype(BF16)
        z_nat[i] = turned(z_row)

        @pl.when((lax.rem(i, 4) == 0) & (i > 0))
        def _():
            for p in range(1, n_dev):
                turn_copy(me, i // 4 - 1, p, peers[p - 1], peers[p - 1]).start()

    own = pltpu.make_async_copy(z_nat.at[:, pl.ds(spot, rows), :], r_buf.at[me], own_sem)
    own.start()
    for p in range(1, n_dev):
        turn_copy(me, rows // 4 - 1, p, peers[p - 1], peers[p - 1]).start()
    own.wait()

    def whole(source, p, target):
        return pltpu.make_async_remote_copy(src_ref=r_buf.at[source], dst_ref=r_buf.at[source], send_sem=t_send.at[p - 1], recv_sem=t_recv.at[p - 1], device_id={'dap': target}, device_id_type=MESH)

    def place(source):
        pad = rows + 8
        for i in range(rows):
            stage[i * pad:i * pad + rows, :] = r_buf[source, i].astype(F32)
        for j in range(rows):
            placed_values = stage[pl.ds(j, rows, stride=pad), :].astype(BF16)
            if last:
                out_ref[j, pl.ds(pl.multiple_of(source * rows, rows), rows), :] = placed_values
            else:
                q_all[j, pl.ds(pl.multiple_of(source * rows, rows), rows), :] = placed_values

    q_all = k_s
    place(me)

    @pl.loop(1, n_dev)
    def _(p):
        source = lax.rem(me + n_dev - p, n_dev)
        whole(source, p, lax.rem(me + p, n_dev)).wait_recv()
        place(source)

    if not last:
        @pl.loop(0, rows)
        def _(j):
            out_ref[j] = turned(q_all[j])

    for p in range(1, n_dev):
        whole(me, p, peers[p - 1]).wait_send()
        bias_copy(me, p, peers[p - 1]).wait_send()
        if share:
            kv_copy(me, p, peers[p - 1]).wait_send()
            kv_copy(lax.rem(me + n_dev - p, n_dev), p, peers[p - 1]).wait_recv()
    if share:
        kv_all[...] = kv_buf[...]


def tri_att(layer, n_dev, cid, last, z, mask_c, w_qkvg, bias_t, heads, w_out, pt=(), kv=None):
    rows, channels, tokens = z.shape
    vmem = pl.BlockSpec(memory_space=pltpu.VMEM)
    dma = pltpu.SemaphoreType.DMA
    share = kv is not None
    scratch = [
        pltpu.VMEM((rows, channels, tokens), BF16),
        pltpu.VMEM((2, rows * 8, LANES), F32),
        pltpu.VMEM((heads, tokens, tokens), BF16),
        pltpu.VMEM((heads, tokens, tokens), F32),
        pltpu.VMEM((4 * channels, channels), BF16),
        pltpu.VMEM((channels, channels), BF16),
        pltpu.VMEM((rows, tokens, channels), BF16),
        pltpu.VMEM((rows, channels, tokens), BF16),
        pltpu.VMEM((rows, channels, tokens), BF16),
        pltpu.VMEM((rows, channels, tokens), F32),
        pltpu.VMEM((rows, tokens, channels), BF16),
        pltpu.VMEM((n_dev, rows, rows, channels), BF16),
        pltpu.VMEM((rows * (rows + 8), LANES), F32),
        dma((n_dev - 1,)), dma((n_dev - 1,)), dma((n_dev - 1,)), dma((n_dev - 1,)), dma,
    ]
    if pt:
        scratch += [pltpu.VMEM(pt[0].shape[:0:-1], BF16), pltpu.VMEM(pt[1].shape[:0:-1], BF16)]
    shape = jax.ShapeDtypeStruct((rows, tokens, channels) if last else z.shape, BF16)
    if share:
        kv_shape = jax.ShapeDtypeStruct((tokens, kv.shape[1]), BF16)
        scratch += [pltpu.VMEM(kv_shape.shape, BF16), dma((n_dev - 1,)), dma((n_dev - 1,))]
    return pl.pallas_call(
        functools.partial(tri_att_kernel, layer, n_dev, heads, last, bool(pt), share),
        out_shape=(shape, kv_shape) if share else shape,
        in_specs=[vmem] * (5 + len(pt) + share),
        out_specs=(vmem, vmem) if share else vmem,
        scratch_shapes=scratch,
        compiler_params=pltpu.CompilerParams(collective_id=cid, has_side_effects=True, vmem_limit_bytes=VMEM_LIMIT),
        name=f'tri_att_{cid}',
    )(z, mask_c, w_qkvg, bias_t, w_out, *pt, *((kv,) if share else ()))


def transition(act_in, w_in, w_out):
    hidden = w_out.shape[0]
    projected = jnp.dot(layer_norm(act_in), w_in, preferred_element_type=F32)
    inner = (jax.nn.silu(projected[..., :hidden]) * projected[..., hidden:]).astype(BF16)
    return (act_in.astype(F32) + jnp.dot(inner, w_out, preferred_element_type=F32)).astype(BF16)


def single_inputs(single, w_qkvg):
    width = w_qkvg.shape[1] // 4
    projected = jnp.dot(layer_norm(single), w_qkvg, preferred_element_type=F32)
    return projected[:, :width].astype(BF16), projected[:, width:3 * width].astype(BF16), jax.nn.sigmoid(projected[:, 3 * width:])


def single_step(single, query, gate, kv_all, pair_bias, mask_all, w_out, st_in, st_out):
    rows, tokens = single.shape[0], kv_all.shape[0]
    heads = pair_bias.shape[1]
    head_dim = query.shape[1] // heads
    query, gate = query.reshape(rows, heads, head_dim), gate.reshape(rows, heads, head_dim)
    kv_all = kv_all.reshape(tokens, 2, heads, head_dim)
    logits = jnp.einsum('ihd,jhd->ihj', query, kv_all[:, 0], preferred_element_type=F32) * head_dim ** -0.5 + pair_bias.astype(F32) + (mask_all.astype(F32) - 1.0) * NEG_BIG
    soft_scores = jax.nn.softmax(logits, axis=-1).astype(BF16)
    attended = jnp.einsum('ihj,jhd->ihd', soft_scores, kv_all[:, 1], preferred_element_type=F32)
    merged = (attended * gate).astype(BF16).reshape(rows, -1)
    single = (single.astype(F32) + jnp.dot(merged, w_out, preferred_element_type=F32)).astype(BF16)
    return transition(single, st_in, st_out)


def solution(mesh):
    row_spec = P(('req', 'dap'))
    single_spec = P(('req', 'dap'), None)
    pair_spec = P(('req', 'dap'), None, None)
    n_dev = mesh.shape['dap']

    def local_program(single, pair, token_mask, *weights):
        w = dict(zip(WEIGHT_NAMES, weights))
        blocks = weights[0].shape[0]
        mask_all = lax.all_gather(token_mask, 'dap', tiled=True)
        tokens = mask_all.shape[0]
        mask_f = mask_all.astype(F32)
        mask_v = mask_f.reshape(2, 1, tokens // 2)
        mask_c = jnp.broadcast_to(((mask_f - 1.0) * NEG_BIG)[:, None], (tokens, LANES))
        heads = w['tas_bias'].shape[2]

        def bias_rows(name):
            swapped = jnp.swapaxes(w[name], 1, 2)
            return jnp.pad(swapped, ((0, 0), (0, 8 - heads), (0, 0)))

        tas_bias, tae_bias = bias_rows('tas_bias'), bias_rows('tae_bias')
        pair = jnp.swapaxes(pair, 1, 2)
        for b in range(blocks):
            cid = 4 * b
            last = b == blocks - 1
            query, kv, gate = single_inputs(single, w['ap_qkvg'][b])
            pair = tri_mult('row', b, n_dev, cid, pair, mask_f, mask_v, w['tmo_proj'], w['tmo_gate'], w['tmo_out'])
            pair = tri_mult('col', b, n_dev, cid + 1, pair, mask_f, mask_v, w['tmi_proj'], w['tmi_gate'], w['tmi_out'])
            pair, kv_all = tri_att(b, n_dev, cid + 2, False, pair, mask_c, w['tas_qkvg'], tas_bias, heads, w['tas_out'], (), kv)
            pair = tri_att(b, n_dev, cid + 3, last, pair, mask_c, w['tae_qkvg'], tae_bias, heads, w['tae_out'], (w['pt_in'], w['pt_out']))
            if last:
                pair_bias = jnp.einsum('ijc,ch->ihj', layer_norm(pair), w['ap_bias'][b], preferred_element_type=F32).astype(BF16)
            else:
                centred = pair.astype(F32) - jnp.mean(pair.astype(F32), axis=1, keepdims=True)
                normed = (centred * lax.rsqrt(jnp.mean(centred * centred, axis=1, keepdims=True) + EPS)).astype(BF16)
                pair_bias = jnp.einsum('icj,ch->ihj', normed, w['ap_bias'][b], preferred_element_type=F32).astype(BF16)
            single = single_step(single, query, gate, kv_all, pair_bias, mask_all, w['ap_out'][b], w['st_in'][b], w['st_out'][b])
        return single, pair

    return jax.shard_map(local_program, mesh=mesh, in_specs=(single_spec, pair_spec, row_spec) + (P(),) * len(WEIGHT_NAMES), out_specs=(single_spec, pair_spec), check_vma=False)
```

```python
import functools

import jax
import jax.numpy as jnp
from jax import lax
from jax.experimental import pallas as pl
from jax.experimental.pallas import tpu as pltpu
from jax.sharding import PartitionSpec as P

EPS = 1e-5
NEG_BIG = 1e9
LOG2E = 1.4426950408889634
F32 = jnp.float32
BF16 = jnp.bfloat16
MESH = pl.DeviceIdType.MESH
WEIGHT_NAMES = ('tmo_proj', 'tmo_gate', 'tmo_out', 'tmi_proj', 'tmi_gate', 'tmi_out', 'tas_qkvg', 'tas_bias', 'tas_out', 'tae_qkvg', 'tae_bias', 'tae_out', 'pt_in', 'pt_out', 'ap_qkvg', 'ap_bias', 'ap_out', 'st_in', 'st_out')
LANES = 128
TURN = 2
VMEM_LIMIT = 60 * 1024 * 1024


def dot_nn(lhs, rhs):
    return lax.dot_general(lhs, rhs, (((1,), (0,)), ((), ())), preferred_element_type=F32)


def turned(values):
    return values.astype(F32).T.astype(BF16)


def dot_nt(lhs, rhs):
    return lax.dot_general(lhs, rhs, (((1,), (1,)), ((), ())), preferred_element_type=F32)


def dot_tn(lhs, rhs):
    return lax.dot_general(lhs, rhs, (((0,), (0,)), ((), ())), preferred_element_type=F32)


def sigmoid(values):
    return 0.5 * jnp.tanh(0.5 * values) + 0.5


def layer_norm_t(values):
    values = values.astype(F32)
    centred = values - jnp.mean(values, axis=0, keepdims=True)
    variance = jnp.mean(centred * centred, axis=0, keepdims=True)
    return (centred * lax.rsqrt(variance + EPS)).astype(BF16)


def layer_norm(values):
    values = values.astype(F32)
    centred = values - jnp.mean(values, axis=-1, keepdims=True)
    variance = jnp.mean(centred * centred, axis=-1, keepdims=True)
    return (centred * lax.rsqrt(variance + EPS)).astype(BF16)


def tri_mult_kernel(kind, layer, n_dev, first, heads, z_hbm, mask_ref, w_proj, w_gate, w_out, *rest):
    rest = list(rest)
    bias_t = rest.pop(0) if heads else None
    out_ref = rest.pop(0)
    mask_out = rest.pop(0) if first else None
    bias_out = rest.pop(0) if heads else None
    mask_send, mask_recv = (rest.pop(), rest.pop()) if first else (None, None)
    if kind == 'row':
        (zfull, b_full, a_full, stage, w_t, x_buf, x_in, mask_l, in_sem, right_send, right_recv, left_send, left_recv, pair_send, pair_recv, x_send, x_recv) = rest
    else:
        (zfull, b_full, a_full, a_turn, stage, w_t, x_buf, x_in, mask_l, in_sem, right_send, right_recv, left_send, left_recv, pair_send, pair_recv, x_send, x_recv) = rest
    chips = n_dev // 2
    rows = zfull.shape[2]
    half_c = b_full.shape[0]
    channels = 2 * half_c
    pad = half_c + 8
    me = lax.axis_index('dap')
    chip, core = me // 2, lax.rem(me, 2)
    partner = chip * 2 + 1 - core
    right = lax.rem(chip + 1, chips) * 2 + core
    left = lax.rem(chip + chips - 1, chips) * 2 + core

    loads = [pltpu.make_async_copy(z_hbm.at[:, :, pl.ds(h * LANES, LANES)], zfull.at[me, h], in_sem.at[h]) for h in range(2)]
    for load in loads:
        load.start()
    barrier = pltpu.get_barrier_semaphore()
    greeted = [lax.rem(me + p, n_dev) for p in range(1, n_dev)] if first else [left, right, partner]
    for peer in greeted:
        pl.semaphore_signal(barrier, inc=1, device_id={'dap': peer}, device_id_type=MESH)
    for load in loads:
        load.wait()
    pl.semaphore_wait(barrier, len(greeted))

    def send(block, half, send_sem, recv_sem, target):
        return pltpu.make_async_remote_copy(src_ref=zfull.at[block, half], dst_ref=zfull.at[block, half], send_sem=send_sem, recv_sem=recv_sem, device_id={'dap': target}, device_id_type=MESH)

    send(me, 0, right_send.at[0], right_recv.at[0], right).start()
    send(me, 1, left_send.at[0], left_recv.at[0], left).start()
    send(me, 1, right_send.at[1], right_recv.at[1], right).start()
    send(me, 0, left_send.at[1], left_recv.at[1], left).start()
    send(me, 0, pair_send.at[0], pair_recv.at[0], partner).start()
    send(me, 1, pair_send.at[1], pair_recv.at[1], partner).start()

    def mask_copy(owner, p, target):
        return pltpu.make_async_remote_copy(src_ref=mask_ref, dst_ref=mask_out.at[pl.ds(pl.multiple_of(owner * rows, rows), rows), :], send_sem=mask_send.at[p - 1], recv_sem=mask_recv.at[p - 1], device_id={'dap': target}, device_id_type=MESH)

    if first:
        for p in range(1, n_dev):
            mask_copy(me, p, greeted[p - 1]).start()
        mask_out[pl.ds(pl.multiple_of(me * rows, rows), rows), :] = mask_ref[...]
    masks = mask_out if first else mask_ref

    x_buf[0, 0, :4 * channels, :] = w_proj[layer].astype(F32).T
    for spot, part in enumerate((2, 3, 0, 1)):
        w_t[spot * half_c:(spot + 1) * half_c, :] = x_buf[0, 0, pl.ds(pl.multiple_of(part * channels + core * half_c, half_c), half_c), :].astype(BF16)

    my_half = chip // (chips // 2)
    my_off = pl.multiple_of(lax.rem(chip, chips // 2) * 2 * rows, 2 * rows)

    def project(block, half, operands):
        weights = w_t[:operands * channels, :]

        @pl.loop(0, rows // 2)
        def _(pair):
            normed = jnp.concatenate([layer_norm_t(zfull[block, half, 2 * pair + t]) for t in range(2)], axis=1)
            slab = dot_nn(weights, normed)
            for o in range(operands):
                gated = sigmoid(slab[o * channels + half_c:(o + 1) * channels]) * slab[o * channels:o * channels + half_c]
                for t in range(2):
                    row = 2 * pair + t
                    stage[o, pl.ds(pl.multiple_of(row * pad, 8), half_c), :] = gated[:, t * LANES:(t + 1) * LANES]

        spot = pl.multiple_of(block * rows, rows)

        @pl.loop(0, half_c // 16)
        def _(group):
            for t in range(16):
                c = group * 16 + t
                b_full[c, half, pl.ds(spot, rows), :] = stage[0, pl.ds(c, rows, stride=pad), :].astype(BF16)
                if operands == 2:
                    left_operand = stage[1, pl.ds(c, rows, stride=pad), :].astype(BF16)
                    if kind == 'row':
                        a_full[c, half, pl.ds(pl.multiple_of(lax.rem(block, 2) * rows, rows), rows), :] = left_operand
                    else:
                        a_full[c, pl.ds(spot, rows), :] = left_operand

    def process(block, half, mine):
        if kind == 'row':
            project(block, half, 2 if mine else 1)
        else:
            @pl.when(half == my_half)
            def _():
                project(block, half, 2)

            @pl.when(half != my_half)
            def _():
                project(block, half, 1)

    @pl.loop(0, 4)
    def _(t):
        who, half = t // 2, lax.rem(t, 2)
        block = jnp.where(who == 0, me, partner)

        @pl.when(who == 1)
        def _():
            send(partner, half, pair_send.at[half], pair_recv.at[half], partner).wait_recv()

        process(block, half, True)

    events = chips - 1

    @pl.loop(0, events)
    def _(e):
        dist = e // 2 + 1
        half_r = lax.rem(e, 2)
        half_l = 1 - half_r
        from_left = lax.rem(chip - dist + chips, chips)
        from_right = lax.rem(chip + dist, chips)
        block_r, block_l = from_left * 2 + core, from_right * 2 + core
        send(block_r, half_r, right_send.at[e], right_recv.at[e], right).wait_recv()

        @pl.when(e + 2 < events)
        def _():
            send(block_r, half_r, right_send.at[e + 2], right_recv.at[e + 2], right).start()

        send(block_r, half_r, pair_send.at[2 * e + 2], pair_recv.at[2 * e + 2], partner).start()
        send(block_l, half_l, left_send.at[e], left_recv.at[e], left).wait_recv()

        @pl.when(e + 2 < events)
        def _():
            send(block_l, half_l, left_send.at[e + 2], left_recv.at[e + 2], left).start()

        send(block_l, half_l, pair_send.at[2 * e + 3], pair_recv.at[2 * e + 3], partner).start()

        @pl.loop(0, 4)
        def _(t):
            side, other = lax.rem(t, 2), t // 2
            owner = jnp.where(other == 0, core, 1 - core)
            block = jnp.where(side == 0, from_left, from_right) * 2 + owner
            half = jnp.where(side == 0, half_r, half_l)

            @pl.when(other == 1)
            def _():
                send(block, half, pair_send.at[2 * e + 2 + side], pair_recv.at[2 * e + 2 + side], partner).wait_recv()

            process(block, half, False)

    if first:
        for p in range(1, n_dev):
            mask_copy(lax.rem(me + n_dev - p, n_dev), p, greeted[p - 1]).wait_recv()
    for half in range(2):
        mask_l[half] = masks[half * LANES:(half + 1) * LANES, :].T[:8, :]
    key_mask = jnp.concatenate([mask_l[0, :1, :], mask_l[1, :1, :]], axis=1).astype(BF16)
    if kind != 'row':
        @pl.loop(0, half_c // 4)
        def _(group):
            for t in range(4):
                a_turn[group * 4 + t] = a_full[group * 4 + t].T

    def exchange(half):
        return pltpu.make_async_remote_copy(src_ref=x_buf.at[1 - core, half], dst_ref=x_in.at[half], send_sem=x_send.at[half], recv_sem=x_recv.at[half], device_id={'dap': partner}, device_id_type=MESH)

    for half in range(2):
        @pl.loop(0, half_c // 4)
        def _(group):
            for t in range(4):
                c = group * 4 + t
                if kind == 'row':
                    lanes = slice(half * LANES, (half + 1) * LANES)
                    product = dot_nt(jnp.concatenate([a_full[c, 0], a_full[c, 1]], axis=1) * key_mask, jnp.concatenate([b_full[c, 0, lanes, :], b_full[c, 1, lanes, :]], axis=1))
                else:
                    product = dot_nn(a_turn[c, pl.ds(my_off, 2 * rows), :] * key_mask, b_full[c, half])
                for who in range(2):
                    x_buf[who, half, pl.ds(c, rows, stride=pad), :] = product[who * rows:(who + 1) * rows, :]

        if half == 0:
            w_own = w_out[layer, pl.ds(pl.multiple_of(core * half_c, half_c), half_c), :]
            w_other = w_out[layer, pl.ds(pl.multiple_of((1 - core) * half_c, half_c), half_c), :]
            w_t[:channels, :] = turned(jnp.concatenate([w_own, w_other], axis=0))
            w_t[channels:2 * channels, :] = turned(w_gate[layer])
        exchange(half).start()

    for half in range(2):
        exchange(half).wait_recv()

        @pl.loop(0, rows)
        def _(i):
            lanes = slice(half * LANES, (half + 1) * LANES)
            spot = pl.ds(pl.multiple_of(i * pad, 8), half_c)
            x_mask = mask_l[half, :1, :] * masks[pl.ds(me * rows + i, 1), :]
            x = jnp.concatenate([x_buf[core, half, spot, :], x_in[half, spot, :]], axis=0) * x_mask
            update = dot_nn(w_t[:channels, :], layer_norm_t(x))
            z_row = zfull[me, half, i]
            gate = sigmoid(dot_nn(w_t[channels:2 * channels, :], layer_norm_t(z_row)))
            z_new = (z_row.astype(F32) + gate * update).astype(BF16)
            out_ref[i, :, lanes] = z_new
            if heads:
                stage[0, pl.ds(pl.multiple_of((half * rows + i) * 8, 8), 8), :] = dot_nn(bias_t[layer], layer_norm_t(z_new))

    if heads:
        for half in range(2):
            for h in range(heads):
                bias_out[h, :, half * LANES:(half + 1) * LANES] = stage[0, pl.ds(half * rows * 8 + h, rows, stride=8), :].astype(BF16)
    for e in range(events):
        send(me, 0, right_send.at[e], right_recv.at[e], right).wait_send()
        send(me, 0, left_send.at[e], left_recv.at[e], left).wait_send()
    for e in range(2 * events + 2):
        send(me, 0, pair_send.at[e], pair_recv.at[e], partner).wait_send()
    for half in range(2):
        exchange(half).wait_send()
    if first:
        for p in range(1, n_dev):
            mask_copy(me, p, greeted[p - 1]).wait_send()


def tri_mult(kind, layer, n_dev, cid, first, z, mask, w_proj, w_gate, w_out, bias_t=None, heads=0):
    rows, channels, tokens = z.shape
    assert tokens == 2 * LANES and channels == LANES and rows * n_dev == tokens
    half_c = channels // 2
    pad = half_c + 8
    events = n_dev // 2 - 1
    vmem = pl.BlockSpec(memory_space=pltpu.VMEM)
    dma = pltpu.SemaphoreType.DMA
    left_operand = [pltpu.VMEM((half_c, 2, 2 * rows, LANES), BF16)]
    shapes = [jax.ShapeDtypeStruct(z.shape, BF16)]
    if first:
        shapes.append(jax.ShapeDtypeStruct((tokens, LANES), F32))
    if heads:
        shapes.append(jax.ShapeDtypeStruct((heads, rows, tokens), BF16))
    if kind != 'row':
        left_operand = [pltpu.VMEM((half_c, tokens, LANES), BF16), pltpu.VMEM((half_c, LANES, tokens), BF16)]
    return pl.pallas_call(
        functools.partial(tri_mult_kernel, kind, layer, n_dev, first, heads),
        out_shape=shapes,
        in_specs=[pl.BlockSpec(memory_space=pl.ANY)] + [vmem] * (4 + bool(heads)),
        out_specs=[vmem] * len(shapes),
        scratch_shapes=[
            pltpu.VMEM((n_dev, 2, rows, channels, LANES), BF16),
            pltpu.VMEM((half_c, 2, tokens, LANES), BF16),
            *left_operand,
            pltpu.VMEM((2, rows * pad, LANES), F32),
            pltpu.VMEM((2 * channels, channels), BF16),
            pltpu.VMEM((2, 2, rows * pad, LANES), F32),
            pltpu.VMEM((2, rows * pad, LANES), F32),
            pltpu.VMEM((2, 8, LANES), F32),
            dma((2,)), dma((events,)), dma((events,)), dma((events,)), dma((events,)), dma((2 * events + 2,)), dma((2 * events + 2,)), dma((2,)), dma((2,)),
        ] + [dma((n_dev - 1,)), dma((n_dev - 1,))] * first,
        compiler_params=pltpu.CompilerParams(collective_id=cid, has_side_effects=True, vmem_limit_bytes=VMEM_LIMIT),
        name=f'tri_mult_{kind}_{cid}',
    )(z, mask, w_proj, w_gate, w_out, *((bias_t,) if heads else ()))


def tri_att_kernel(layer, n_dev, heads, last, trans, share, z_ref, mask_ref, w_qkvg, bias_own, w_out, *rest):
    rest = list(rest)
    pt_in, pt_out = (rest.pop(0), rest.pop(0)) if trans else (None, None)
    kv_in, bias_t = (rest.pop(0), rest.pop(0)) if share else (None, None)
    out_ref = rest.pop(0)
    kv_all, bias_next = (rest.pop(0), rest.pop(0)) if share else (None, None)
    (bias_s, bias_all, logit_bias, w_t, w_o, k_s, q_s, v_s, g_s, z_nat, r_buf, stage, b_send, b_recv, d_send, d_recv, t_send, t_recv, own_sem) = rest[:19]
    rest = rest[19:]
    pt_in_t, pt_out_t = (rest.pop(0), rest.pop(0)) if trans else (None, None)
    kv_send, kv_recv = (rest.pop(0), rest.pop(0)) if share else (None, None)
    rows, channels, tokens = z_ref.shape
    width = channels // heads
    me = lax.axis_index('dap')
    barrier = pltpu.get_barrier_semaphore()
    peers = [lax.rem(me + p, n_dev) for p in range(1, n_dev)]
    for peer in peers:
        pl.semaphore_signal(barrier, inc=1, device_id={'dap': peer}, device_id_type=MESH)

    chips = n_dev // 2
    chip, core = me // 2, lax.rem(me, 2)
    partner = chip * 2 + 1 - core
    spot = pl.multiple_of(me * rows, rows)

    def rows_of(ref, owner, lead):
        block = pl.ds(pl.multiple_of(owner * rows, rows), rows)
        return ref.at[:, block, :] if lead else ref.at[block, :]

    def bias_copy(owner, d, target):
        return pltpu.make_async_remote_copy(src_ref=bias_own, dst_ref=rows_of(bias_all, owner, True), send_sem=b_send.at[d], recv_sem=b_recv.at[d], device_id={'dap': target}, device_id_type=MESH)

    def relay_copy(owner, d):
        ref = rows_of(bias_all, owner, True)
        return pltpu.make_async_remote_copy(src_ref=ref, dst_ref=ref, send_sem=d_send.at[d], recv_sem=d_recv.at[d], device_id={'dap': partner}, device_id_type=MESH)

    def kv_copy(owner, p, target):
        return pltpu.make_async_remote_copy(src_ref=kv_in, dst_ref=rows_of(kv_all, owner, False), send_sem=kv_send.at[p - 1], recv_sem=kv_recv.at[p - 1], device_id={'dap': target}, device_id_type=MESH)

    def chip_core(d):
        return lax.rem(chip + d + chips, chips) * 2 + core

    pl.semaphore_wait(barrier, n_dev - 1)
    for d in range(chips):
        bias_copy(me, d, partner if d == 0 else chip_core(d)).start()
    if share:
        for p in range(1, n_dev):
            kv_copy(me, p, peers[p - 1]).start()
        kv_all[pl.ds(spot, rows), :] = kv_in[...]
    bias_all[:, pl.ds(spot, rows), :] = bias_own[...]
    w_t[...] = turned(w_qkvg[layer])
    w_o[...] = turned(w_out[layer])
    if trans:
        for part in range(0, pt_in_t.shape[0], channels):
            pt_in_t[part:part + channels, :] = turned(pt_in[layer, :, part:part + channels])
        pt_out_t[...] = turned(pt_out[layer])

    def projections(i):
        slab = dot_nn(w_t[...], layer_norm_t(z_ref[i]))
        q_s[i] = slab[:channels].astype(BF16)
        k_s[i] = slab[channels:2 * channels].T.astype(BF16)
        v_s[i] = slab[2 * channels:3 * channels].astype(BF16)
        g_s[i] = sigmoid(slab[3 * channels:])

    @pl.loop(0, rows // 2)
    def _(pair):
        projections(2 * pair)
        projections(2 * pair + 1)

    for d in range(1, chips):
        bias_copy(chip_core(-d), d, partner).wait_recv()
        relay_copy(chip_core(-d), d).start()
    bias_copy(partner, 0, partner).wait_recv()
    for d in range(1, chips):
        relay_copy(lax.rem(chip - d + chips, chips) * 2 + 1 - core, d).wait_recv()
    for h in range(heads):
        for qh in range(2):
            for kh in range(2):
                keys, queries = slice(kh * LANES, (kh + 1) * LANES), slice(qh * LANES, (qh + 1) * LANES)
                tile = bias_all[h, queries, keys].astype(F32).T if share else bias_all[h, keys, queries].astype(F32)
                logit_bias[h, keys, queries] = (tile + (mask_ref[keys, :] - 1.0) * NEG_BIG) * LOG2E
    scale = width ** -0.5 * LOG2E

    def turn_copy(source, t, p, target, to):
        return pltpu.make_async_remote_copy(
            src_ref=z_nat.at[pl.ds(TURN * t, TURN), pl.ds(pl.multiple_of(to * rows, rows), rows), :], dst_ref=r_buf.at[source, pl.ds(TURN * t, TURN)],
            send_sem=t_send.at[p - 1], recv_sem=t_recv.at[p - 1], device_id={'dap': target}, device_id_type=MESH)

    @pl.loop(0, rows)
    def _(i):
        keys = k_s[i]
        parts = []
        for h in range(heads):
            pieces = [q_s[i, h * width:(h + 1) * width, :]]
            if h:
                pieces = [jnp.zeros((h * width, tokens), BF16)] + pieces
            if h < heads - 1:
                pieces = pieces + [jnp.zeros(((heads - 1 - h) * width, tokens), BF16)]
            scores = dot_nn(keys, jnp.concatenate(pieces, axis=0))
            halves = []
            for qh in range(2):
                lanes = slice(qh * LANES, (qh + 1) * LANES)
                logits = scores[:, lanes] * scale + logit_bias[h, :, lanes]
                weights = jnp.exp2(logits - jnp.max(logits, axis=0, keepdims=True))
                total = jnp.sum(weights, axis=0, keepdims=True)
                halves.append((weights * (1.0 / total)).astype(BF16))
            parts.append(dot_nn(v_s[i, h * width:(h + 1) * width, :], jnp.concatenate(halves, axis=1)))
        merged = (jnp.concatenate(parts, axis=0) * g_s[i]).astype(BF16)
        z_row = (z_ref[i].astype(F32) + dot_nn(w_o[...], merged)).astype(BF16)
        if trans:
            normed = layer_norm_t(z_row)
            hidden = pt_out.shape[1]
            update = jnp.zeros((channels, tokens), F32)
            for part in range(0, hidden, channels):
                first = dot_nn(pt_in_t[part:part + channels, :], normed)
                second = dot_nn(pt_in_t[hidden + part:hidden + part + channels, :], normed)
                update = update + dot_nn(pt_out_t[:, part:part + channels], (first * sigmoid(first) * second).astype(BF16))
            z_row = (z_row.astype(F32) + update).astype(BF16)
        z_nat[i] = turned(z_row)

        if share:
            bias_s[0, pl.ds(pl.multiple_of(i * 8, 8), 8), :], bias_s[1, pl.ds(pl.multiple_of(i * 8, 8), 8), :] = jnp.split(dot_nn(bias_t[layer], layer_norm_t(z_row)), 2, axis=1)

        @pl.when((lax.rem(i, TURN) == 0) & (i > 0))
        def _():
            for p in range(1, n_dev):
                turn_copy(me, i // TURN - 1, p, peers[p - 1], peers[p - 1]).start()

    own = pltpu.make_async_copy(z_nat.at[:, pl.ds(spot, rows), :], r_buf.at[me], own_sem)
    own.start()
    for p in range(1, n_dev):
        turn_copy(me, rows // TURN - 1, p, peers[p - 1], peers[p - 1]).start()
    own.wait()

    def whole(source, p, target):
        return pltpu.make_async_remote_copy(src_ref=r_buf.at[source], dst_ref=r_buf.at[source], send_sem=t_send.at[p - 1], recv_sem=t_recv.at[p - 1], device_id={'dap': target}, device_id_type=MESH)

    def place(source):
        pad = rows + 8
        for i in range(rows):
            stage[i * pad:i * pad + rows, :] = r_buf[source, i].astype(F32)
        for j in range(rows):
            placed_values = stage[pl.ds(j, rows, stride=pad), :].astype(BF16)
            if last:
                out_ref[j, pl.ds(pl.multiple_of(source * rows, rows), rows), :] = placed_values
            else:
                q_all[j, pl.ds(pl.multiple_of(source * rows, rows), rows), :] = placed_values

    q_all = k_s
    place(me)

    @pl.loop(1, n_dev)
    def _(p):
        source = lax.rem(me + n_dev - p, n_dev)
        whole(source, p, lax.rem(me + p, n_dev)).wait_recv()
        place(source)

    if not last:
        @pl.loop(0, rows)
        def _(j):
            out_ref[j] = turned(q_all[j])

    for p in range(1, n_dev):
        whole(me, p, peers[p - 1]).wait_send()
        if share:
            kv_copy(me, p, peers[p - 1]).wait_send()
            kv_copy(lax.rem(me + n_dev - p, n_dev), p, peers[p - 1]).wait_recv()
    for d in range(chips):
        bias_copy(me, d, partner).wait_send()
        if d:
            relay_copy(chip_core(-d), d).wait_send()
    if share:
        for h in range(heads):
            for half in range(2):
                bias_next[h, :, half * LANES:(half + 1) * LANES] = bias_s[half, pl.ds(h, rows, stride=8), :].astype(BF16)


def tri_att(layer, n_dev, cid, last, z, mask, w_qkvg, bias_own, w_out, pt=(), kv=None, bias_t=None):
    rows, channels, tokens = z.shape
    vmem = pl.BlockSpec(memory_space=pltpu.VMEM)
    dma = pltpu.SemaphoreType.DMA
    share = kv is not None
    heads = bias_own.shape[0]
    scratch = [
        pltpu.VMEM((2, rows * 8, LANES), F32),
        pltpu.VMEM((heads, tokens, tokens), BF16),
        pltpu.VMEM((heads, tokens, tokens), F32),
        pltpu.VMEM((4 * channels, channels), BF16),
        pltpu.VMEM((channels, channels), BF16),
        pltpu.VMEM((rows, tokens, channels), BF16),
        pltpu.VMEM((rows, channels, tokens), BF16),
        pltpu.VMEM((rows, channels, tokens), BF16),
        pltpu.VMEM((rows, channels, tokens), F32),
        pltpu.VMEM((rows, tokens, channels), BF16),
        pltpu.VMEM((n_dev, rows, rows, channels), BF16),
        pltpu.VMEM((rows * (rows + 8), LANES), F32),
        dma((n_dev // 2,)), dma((n_dev // 2,)), dma((n_dev // 2,)), dma((n_dev // 2,)), dma((n_dev - 1,)), dma((n_dev - 1,)), dma,
    ]
    if pt:
        scratch += [pltpu.VMEM(pt[0].shape[:0:-1], BF16), pltpu.VMEM(pt[1].shape[:0:-1], BF16)]
    shape = jax.ShapeDtypeStruct((rows, tokens, channels) if last else z.shape, BF16)
    if share:
        kv_shape = jax.ShapeDtypeStruct((tokens, kv.shape[1]), BF16)
        scratch += [dma((n_dev - 1,)), dma((n_dev - 1,))]
        bias_shape = jax.ShapeDtypeStruct(bias_own.shape, BF16)
    return pl.pallas_call(
        functools.partial(tri_att_kernel, layer, n_dev, heads, last, bool(pt), share),
        out_shape=(shape, kv_shape, bias_shape) if share else shape,
        in_specs=[vmem] * (5 + len(pt) + 2 * share),
        out_specs=(vmem, vmem, vmem) if share else vmem,
        scratch_shapes=scratch,
        compiler_params=pltpu.CompilerParams(collective_id=cid, has_side_effects=True, vmem_limit_bytes=VMEM_LIMIT),
        name=f'tri_att_{cid}',
    )(z, mask, w_qkvg, bias_own, w_out, *pt, *((kv, bias_t) if share else ()))


def transition(act_in, w_in, w_out):
    hidden = w_out.shape[0]
    projected = jnp.dot(layer_norm(act_in), w_in, preferred_element_type=F32)
    inner = (jax.nn.silu(projected[..., :hidden]) * projected[..., hidden:]).astype(BF16)
    return (act_in.astype(F32) + jnp.dot(inner, w_out, preferred_element_type=F32)).astype(BF16)


def single_inputs(single, w_qkvg):
    width = w_qkvg.shape[1] // 4
    projected = jnp.dot(layer_norm(single), w_qkvg, preferred_element_type=F32)
    return projected[:, :width].astype(BF16), projected[:, width:3 * width].astype(BF16), jax.nn.sigmoid(projected[:, 3 * width:])


def single_step(single, query, gate, kv_all, pair_bias, mask_all, w_out, st_in, st_out):
    rows, tokens = single.shape[0], kv_all.shape[0]
    heads = pair_bias.shape[1]
    head_dim = query.shape[1] // heads
    query, gate = query.reshape(rows, heads, head_dim), gate.reshape(rows, heads, head_dim)
    kv_all = kv_all.reshape(tokens, 2, heads, head_dim)
    logits = jnp.einsum('ihd,jhd->ihj', query, kv_all[:, 0], preferred_element_type=F32) * head_dim ** -0.5 + pair_bias.astype(F32) + (mask_all - 1.0) * NEG_BIG
    soft_scores = jax.nn.softmax(logits, axis=-1).astype(BF16)
    attended = jnp.einsum('ihj,jhd->ihd', soft_scores, kv_all[:, 1], preferred_element_type=F32)
    merged = (attended * gate).astype(BF16).reshape(rows, -1)
    single = (single.astype(F32) + jnp.dot(merged, w_out, preferred_element_type=F32)).astype(BF16)
    return transition(single, st_in, st_out)


def solution(mesh):
    row_spec = P(('req', 'dap'))
    single_spec = P(('req', 'dap'), None)
    pair_spec = P(('req', 'dap'), None, None)
    n_dev = mesh.shape['dap']

    def local_program(single, pair, token_mask, *weights):
        w = dict(zip(WEIGHT_NAMES, weights))
        blocks = weights[0].shape[0]
        mask = jnp.broadcast_to(token_mask.astype(F32)[:, None], (token_mask.shape[0], LANES))
        heads = w['tas_bias'].shape[2]

        def bias_rows(name):
            swapped = jnp.swapaxes(w[name], 1, 2)
            return jnp.pad(swapped, ((0, 0), (0, 8 - heads), (0, 0)))

        tas_bias, tae_bias = bias_rows('tas_bias'), bias_rows('tae_bias')
        pair = jnp.swapaxes(pair, 1, 2)
        for b in range(blocks):
            cid = 4 * b
            last = b == blocks - 1
            query, kv, gate = single_inputs(single, w['ap_qkvg'][b])
            out = ('row', b, n_dev, cid, b == 0, pair, mask, w['tmo_proj'], w['tmo_gate'], w['tmo_out'])
            if b == 0:
                pair, mask = tri_mult(*out)
            else:
                pair, = tri_mult(*out)
            pair, bias = tri_mult('col', b, n_dev, cid + 1, False, pair, mask, w['tmi_proj'], w['tmi_gate'], w['tmi_out'], tas_bias, heads)
            pair, kv_all, bias = tri_att(b, n_dev, cid + 2, False, pair, mask, w['tas_qkvg'], bias, w['tas_out'], (), kv, tae_bias)
            pair = tri_att(b, n_dev, cid + 3, last, pair, mask, w['tae_qkvg'], bias, w['tae_out'], (w['pt_in'], w['pt_out']))
            if last:
                pair_bias = jnp.einsum('ijc,ch->ihj', layer_norm(pair), w['ap_bias'][b], preferred_element_type=F32).astype(BF16)
            else:
                centred = pair.astype(F32) - jnp.mean(pair.astype(F32), axis=1, keepdims=True)
                normed = (centred * lax.rsqrt(jnp.mean(centred * centred, axis=1, keepdims=True) + EPS)).astype(BF16)
                pair_bias = jnp.einsum('icj,ch->ihj', normed, w['ap_bias'][b], preferred_element_type=F32).astype(BF16)
            single = single_step(single, query, gate, kv_all, pair_bias, mask[:, 0], w['ap_out'][b], w['st_in'][b], w['st_out'][b])
        return single, pair

    return jax.shard_map(local_program, mesh=mesh, in_specs=(single_spec, pair_spec, row_spec) + (P(),) * len(WEIGHT_NAMES), out_specs=(single_spec, pair_spec), check_vma=False)
```

```python
import functools

import jax
import jax.numpy as jnp
from jax import lax
from jax.experimental import pallas as pl
from jax.experimental.pallas import tpu as pltpu
from jax.sharding import PartitionSpec as P

EPS = 1e-5
NEG_BIG = 1e9
LOG2E = 1.4426950408889634
F32 = jnp.float32
BF16 = jnp.bfloat16
MESH = pl.DeviceIdType.MESH
WEIGHT_NAMES = ('tmo_proj', 'tmo_gate', 'tmo_out', 'tmi_proj', 'tmi_gate', 'tmi_out', 'tas_qkvg', 'tas_bias', 'tas_out', 'tae_qkvg', 'tae_bias', 'tae_out', 'pt_in', 'pt_out', 'ap_qkvg', 'ap_bias', 'ap_out', 'st_in', 'st_out')
LANES = 128
TURN = 2
VMEM_LIMIT = 60 * 1024 * 1024


def dot_nn(lhs, rhs):
    return lax.dot_general(lhs, rhs, (((1,), (0,)), ((), ())), preferred_element_type=F32)


def turned(values):
    return values.astype(F32).T.astype(BF16)


def dot_nt(lhs, rhs):
    return lax.dot_general(lhs, rhs, (((1,), (1,)), ((), ())), preferred_element_type=F32)


def dot_tn(lhs, rhs):
    return lax.dot_general(lhs, rhs, (((0,), (0,)), ((), ())), preferred_element_type=F32)


def sigmoid(values):
    return 0.5 * jnp.tanh(0.5 * values) + 0.5


def layer_norm_t(values):
    values = values.astype(F32)
    centred = values - jnp.mean(values, axis=0, keepdims=True)
    variance = jnp.mean(centred * centred, axis=0, keepdims=True)
    return (centred * lax.rsqrt(variance + EPS)).astype(BF16)


def layer_norm(values):
    values = values.astype(F32)
    centred = values - jnp.mean(values, axis=-1, keepdims=True)
    variance = jnp.mean(centred * centred, axis=-1, keepdims=True)
    return (centred * lax.rsqrt(variance + EPS)).astype(BF16)


def tri_mult_kernel(kind, layer, n_dev, first, heads, z_hbm, mask_ref, w_proj, w_gate, w_out, *rest):
    rest = list(rest)
    bias_t = rest.pop(0) if heads else None
    out_ref = rest.pop(0)
    mask_out = rest.pop(0) if first else None
    bias_out = rest.pop(0) if heads else None
    mask_send, mask_recv = (rest.pop(), rest.pop()) if first else (None, None)
    (zfull, b_full, a_full, a_turn, stage, w_t, w_o, w_g, gate_s, x_buf, x_in, mask_l, in_sem, right_send, right_recv, left_send, left_recv, pair_send, pair_recv, x_send, x_recv) = rest
    chips = n_dev // 2
    rows = zfull.shape[2]
    half_c = b_full.shape[0]
    channels = 2 * half_c
    pad = half_c + 8
    me = lax.axis_index('dap')
    chip, core = me // 2, lax.rem(me, 2)
    partner = chip * 2 + 1 - core
    right = lax.rem(chip + 1, chips) * 2 + core
    left = lax.rem(chip + chips - 1, chips) * 2 + core

    loads = [pltpu.make_async_copy(z_hbm.at[:, :, pl.ds(h * LANES, LANES)], zfull.at[me, h], in_sem.at[h]) for h in range(2)]
    for load in loads:
        load.start()
    barrier = pltpu.get_barrier_semaphore()
    greeted = [lax.rem(me + p, n_dev) for p in range(1, n_dev)] if first else [left, right, partner]
    for peer in greeted:
        pl.semaphore_signal(barrier, inc=1, device_id={'dap': peer}, device_id_type=MESH)
    for load in loads:
        load.wait()
    pl.semaphore_wait(barrier, len(greeted))

    def send(block, half, send_sem, recv_sem, target):
        return pltpu.make_async_remote_copy(src_ref=zfull.at[block, half], dst_ref=zfull.at[block, half], send_sem=send_sem, recv_sem=recv_sem, device_id={'dap': target}, device_id_type=MESH)

    send(me, 0, right_send.at[0], right_recv.at[0], right).start()
    send(me, 1, left_send.at[0], left_recv.at[0], left).start()
    send(me, 1, right_send.at[1], right_recv.at[1], right).start()
    send(me, 0, left_send.at[1], left_recv.at[1], left).start()
    send(me, 0, pair_send.at[0], pair_recv.at[0], partner).start()
    send(me, 1, pair_send.at[1], pair_recv.at[1], partner).start()

    def mask_copy(owner, p, target):
        return pltpu.make_async_remote_copy(src_ref=mask_ref, dst_ref=mask_out.at[pl.ds(pl.multiple_of(owner * rows, rows), rows), :], send_sem=mask_send.at[p - 1], recv_sem=mask_recv.at[p - 1], device_id={'dap': target}, device_id_type=MESH)

    if first:
        for p in range(1, n_dev):
            mask_copy(me, p, greeted[p - 1]).start()
        mask_out[pl.ds(pl.multiple_of(me * rows, rows), rows), :] = mask_ref[...]
    masks = mask_out if first else mask_ref

    x_buf[0, 0, :4 * channels, :] = w_proj[layer].astype(F32).T
    for spot, part in enumerate((2, 3, 0, 1)):
        w_t[spot * half_c:(spot + 1) * half_c, :] = x_buf[0, 0, pl.ds(pl.multiple_of(part * channels + core * half_c, half_c), half_c), :].astype(BF16)

    w_own = w_out[layer, pl.ds(pl.multiple_of(core * half_c, half_c), half_c), :]
    w_other = w_out[layer, pl.ds(pl.multiple_of((1 - core) * half_c, half_c), half_c), :]
    w_o[...] = turned(jnp.concatenate([w_own, w_other], axis=0))
    w_g[...] = turned(w_gate[layer])

    my_half = chip // (chips // 2)
    my_off = pl.multiple_of(lax.rem(chip, chips // 2) * 2 * rows, 2 * rows)

    def project(block, half, operands):
        weights = w_t[:operands * channels, :]

        @pl.loop(0, rows // 2)
        def _(pair):
            normed = jnp.concatenate([layer_norm_t(zfull[block, half, 2 * pair + t]) for t in range(2)], axis=1)
            slab = dot_nn(weights, normed)
            for o in range(operands):
                gated = sigmoid(slab[o * channels + half_c:(o + 1) * channels]) * slab[o * channels:o * channels + half_c]
                for t in range(2):
                    row = 2 * pair + t
                    stage[o, pl.ds(pl.multiple_of(row * pad, 8), half_c), :] = gated[:, t * LANES:(t + 1) * LANES]

        spot = pl.multiple_of(block * rows, rows)

        @pl.loop(0, half_c // 16)
        def _(group):
            for t in range(16):
                c = group * 16 + t
                b_full[c, half, pl.ds(spot, rows), :] = stage[0, pl.ds(c, rows, stride=pad), :].astype(BF16)
                if operands == 2:
                    left_operand = stage[1, pl.ds(c, rows, stride=pad), :].astype(BF16)
                    if kind == 'row':
                        a_full[c, half, pl.ds(pl.multiple_of(lax.rem(block, 2) * rows, rows), rows), :] = left_operand
                    else:
                        a_full[c, pl.ds(spot, rows), :] = left_operand

    def process(block, half, mine):
        if kind == 'row':
            project(block, half, 2 if mine else 1)
        else:
            @pl.when(half == my_half)
            def _():
                project(block, half, 2)

            @pl.when(half != my_half)
            def _():
                project(block, half, 1)

    @pl.loop(0, 4)
    def _(t):
        who, half = t // 2, lax.rem(t, 2)
        block = jnp.where(who == 0, me, partner)

        @pl.when(who == 1)
        def _():
            send(partner, half, pair_send.at[half], pair_recv.at[half], partner).wait_recv()

        process(block, half, True)

    events = chips - 1

    def turn_left():
        key_mask = jnp.concatenate([mask_l[0, :1, :], mask_l[1, :1, :]], axis=1).astype(BF16)

        @pl.loop(0, half_c // 4)
        def _(group):
            for t in range(4):
                c = group * 4 + t
                left_operand = jnp.concatenate([a_full[c, 0], a_full[c, 1]], axis=1) if kind == 'row' else a_full[c].T
                a_turn[c] = left_operand * key_mask

    @pl.loop(0, events)
    def _(e):
        dist = e // 2 + 1
        half_r = lax.rem(e, 2)
        half_l = 1 - half_r
        from_left = lax.rem(chip - dist + chips, chips)
        from_right = lax.rem(chip + dist, chips)
        block_r, block_l = from_left * 2 + core, from_right * 2 + core
        send(block_r, half_r, right_send.at[e], right_recv.at[e], right).wait_recv()

        @pl.when(e + 2 < events)
        def _():
            send(block_r, half_r, right_send.at[e + 2], right_recv.at[e + 2], right).start()

        send(block_r, half_r, pair_send.at[2 * e + 2], pair_recv.at[2 * e + 2], partner).start()
        send(block_l, half_l, left_send.at[e], left_recv.at[e], left).wait_recv()

        @pl.when(e + 2 < events)
        def _():
            send(block_l, half_l, left_send.at[e + 2], left_recv.at[e + 2], left).start()

        send(block_l, half_l, pair_send.at[2 * e + 3], pair_recv.at[2 * e + 3], partner).start()

        @pl.when(e == 0)
        def _():
            @pl.loop(0, rows)
            def _(i):
                for half in range(2):
                    gate_s[half, i] = sigmoid(dot_nn(w_g[...], layer_norm_t(zfull[me, half, i])))

        @pl.when(e == 1)
        def _():
            if first:
                for p in range(1, n_dev):
                    mask_copy(lax.rem(me + n_dev - p, n_dev), p, greeted[p - 1]).wait_recv()
            for half in range(2):
                mask_l[half] = masks[half * LANES:(half + 1) * LANES, :].T[:8, :]
            if kind == 'row':
                turn_left()

        @pl.loop(0, 4)
        def _(t):
            side, other = lax.rem(t, 2), t // 2
            owner = jnp.where(other == 0, core, 1 - core)
            block = jnp.where(side == 0, from_left, from_right) * 2 + owner
            half = jnp.where(side == 0, half_r, half_l)

            @pl.when(other == 1)
            def _():
                send(block, half, pair_send.at[2 * e + 2 + side], pair_recv.at[2 * e + 2 + side], partner).wait_recv()

            process(block, half, False)

    if kind != 'row':
        turn_left()

    def exchange(half):
        return pltpu.make_async_remote_copy(src_ref=x_buf.at[1 - core, half], dst_ref=x_in.at[half], send_sem=x_send.at[half], recv_sem=x_recv.at[half], device_id={'dap': partner}, device_id_type=MESH)

    @pl.loop(0, half_c // 4)
    def _(group):
        for t in range(4):
            c = group * 4 + t
            rhs = jnp.concatenate([b_full[c, 0], b_full[c, 1]], axis=1)
            product = dot_nt(a_turn[c], rhs) if kind == 'row' else dot_nn(a_turn[c, pl.ds(my_off, 2 * rows), :], rhs)
            for who in range(2):
                for half in range(2):
                    x_buf[who, half, pl.ds(c, rows, stride=pad), :] = product[who * rows:(who + 1) * rows, half * LANES:(half + 1) * LANES]

    for e in range(events):
        send(me, 0, right_send.at[e], right_recv.at[e], right).wait_send()
        send(me, 0, left_send.at[e], left_recv.at[e], left).wait_send()
    for half in range(2):
        exchange(half).start()
    for half in range(2):
        exchange(half).wait_recv()

        @pl.loop(0, rows // 2)
        def _(pair):
            lanes = slice(half * LANES, (half + 1) * LANES)
            for t in range(2):
                i = 2 * pair + t
                spot = pl.ds(pl.multiple_of(i * pad, 8), half_c)
                x_mask = mask_l[half, :1, :] * masks[pl.ds(me * rows + i, 1), :]
                x = jnp.concatenate([x_buf[core, half, spot, :], x_in[half, spot, :]], axis=0) * x_mask
                update = dot_nn(w_o[...], layer_norm_t(x))
                z_new = (zfull[me, half, i].astype(F32) + gate_s[half, i] * update).astype(BF16)
                out_ref[i, :, lanes] = z_new
                if heads:
                    stage[0, pl.ds(pl.multiple_of((half * rows + i) * 8, 8), 8), :] = dot_nn(bias_t[layer], layer_norm_t(z_new))

    if heads:
        for half in range(2):
            for h in range(heads):
                bias_out[h, :, half * LANES:(half + 1) * LANES] = stage[0, pl.ds(half * rows * 8 + h, rows, stride=8), :].astype(BF16)
    for e in range(2 * events + 2):
        send(me, 0, pair_send.at[e], pair_recv.at[e], partner).wait_send()
    for half in range(2):
        exchange(half).wait_send()
    if first:
        for p in range(1, n_dev):
            mask_copy(me, p, greeted[p - 1]).wait_send()


def tri_mult(kind, layer, n_dev, cid, first, z, mask, w_proj, w_gate, w_out, bias_t=None, heads=0):
    rows, channels, tokens = z.shape
    assert tokens == 2 * LANES and channels == LANES and rows * n_dev == tokens
    half_c = channels // 2
    pad = half_c + 8
    events = n_dev // 2 - 1
    vmem = pl.BlockSpec(memory_space=pltpu.VMEM)
    dma = pltpu.SemaphoreType.DMA
    left_operand = [pltpu.VMEM((half_c, 2, 2 * rows, LANES), BF16), pltpu.VMEM((half_c, 2 * rows, tokens), BF16)]
    shapes = [jax.ShapeDtypeStruct(z.shape, BF16)]
    if first:
        shapes.append(jax.ShapeDtypeStruct((tokens, LANES), F32))
    if heads:
        shapes.append(jax.ShapeDtypeStruct((heads, rows, tokens), BF16))
    if kind != 'row':
        left_operand = [pltpu.VMEM((half_c, tokens, LANES), BF16), pltpu.VMEM((half_c, LANES, tokens), BF16)]
    return pl.pallas_call(
        functools.partial(tri_mult_kernel, kind, layer, n_dev, first, heads),
        out_shape=shapes,
        in_specs=[pl.BlockSpec(memory_space=pl.ANY)] + [vmem] * (4 + bool(heads)),
        out_specs=[vmem] * len(shapes),
        scratch_shapes=[
            pltpu.VMEM((n_dev, 2, rows, channels, LANES), BF16),
            pltpu.VMEM((half_c, 2, tokens, LANES), BF16),
            *left_operand,
            pltpu.VMEM((2, rows * pad, LANES), F32),
            pltpu.VMEM((2 * channels, channels), BF16),
            pltpu.VMEM((channels, channels), BF16),
            pltpu.VMEM((channels, channels), BF16),
            pltpu.VMEM((2, rows, channels, LANES), F32),
            pltpu.VMEM((2, 2, rows * pad, LANES), F32),
            pltpu.VMEM((2, rows * pad, LANES), F32),
            pltpu.VMEM((2, 8, LANES), F32),
            dma((2,)), dma((events,)), dma((events,)), dma((events,)), dma((events,)), dma((2 * events + 2,)), dma((2 * events + 2,)), dma((2,)), dma((2,)),
        ] + [dma((n_dev - 1,)), dma((n_dev - 1,))] * first,
        compiler_params=pltpu.CompilerParams(collective_id=cid, has_side_effects=True, vmem_limit_bytes=VMEM_LIMIT),
        name=f'tri_mult_{kind}_{cid}',
    )(z, mask, w_proj, w_gate, w_out, *((bias_t,) if heads else ()))


def tri_att_kernel(layer, n_dev, heads, last, trans, share, z_ref, mask_ref, w_qkvg, bias_own, w_out, *rest):
    rest = list(rest)
    pt_in, pt_out = (rest.pop(0), rest.pop(0)) if trans else (None, None)
    kv_in, bias_t = (rest.pop(0), rest.pop(0)) if share else (None, None)
    out_ref = rest.pop(0)
    kv_all, bias_next = (rest.pop(0), rest.pop(0)) if share else (None, None)
    (bias_s, bias_all, logit_bias, w_t, w_o, k_s, q_s, v_s, g_s, z_nat, r_buf, stage, b_send, b_recv, d_send, d_recv, t_send, t_recv, own_sem) = rest[:19]
    rest = rest[19:]
    pt_in_t, pt_out_t = (rest.pop(0), rest.pop(0)) if trans else (None, None)
    kv_send, kv_recv = (rest.pop(0), rest.pop(0)) if share else (None, None)
    rows, channels, tokens = z_ref.shape
    width = channels // heads
    me = lax.axis_index('dap')
    barrier = pltpu.get_barrier_semaphore()
    peers = [lax.rem(me + p, n_dev) for p in range(1, n_dev)]
    for peer in peers:
        pl.semaphore_signal(barrier, inc=1, device_id={'dap': peer}, device_id_type=MESH)

    chips = n_dev // 2
    chip, core = me // 2, lax.rem(me, 2)
    partner = chip * 2 + 1 - core
    spot = pl.multiple_of(me * rows, rows)

    def rows_of(ref, owner, lead):
        block = pl.ds(pl.multiple_of(owner * rows, rows), rows)
        return ref.at[:, block, :] if lead else ref.at[block, :]

    def bias_copy(owner, d, target):
        return pltpu.make_async_remote_copy(src_ref=bias_own, dst_ref=rows_of(bias_all, owner, True), send_sem=b_send.at[d], recv_sem=b_recv.at[d], device_id={'dap': target}, device_id_type=MESH)

    def relay_copy(owner, d):
        ref = rows_of(bias_all, owner, True)
        return pltpu.make_async_remote_copy(src_ref=ref, dst_ref=ref, send_sem=d_send.at[d], recv_sem=d_recv.at[d], device_id={'dap': partner}, device_id_type=MESH)

    def kv_copy(owner, p, target):
        return pltpu.make_async_remote_copy(src_ref=kv_in, dst_ref=rows_of(kv_all, owner, False), send_sem=kv_send.at[p - 1], recv_sem=kv_recv.at[p - 1], device_id={'dap': target}, device_id_type=MESH)

    def chip_core(d):
        return lax.rem(chip + d + chips, chips) * 2 + core

    pl.semaphore_wait(barrier, n_dev - 1)
    for d in range(chips):
        bias_copy(me, d, partner if d == 0 else chip_core(d)).start()
    if share:
        for p in range(1, n_dev):
            kv_copy(me, p, peers[p - 1]).start()
        kv_all[pl.ds(spot, rows), :] = kv_in[...]
    bias_all[:, pl.ds(spot, rows), :] = bias_own[...]
    w_t[...] = turned(w_qkvg[layer])
    w_o[...] = turned(w_out[layer])
    if trans:
        for part in range(0, pt_in_t.shape[0], channels):
            pt_in_t[part:part + channels, :] = turned(pt_in[layer, :, part:part + channels])
        pt_out_t[...] = turned(pt_out[layer])

    def projections(i):
        slab = dot_nn(w_t[...], layer_norm_t(z_ref[i]))
        q_s[i] = slab[:channels].astype(BF16)
        k_s[i] = slab[channels:2 * channels].T.astype(BF16)
        v_s[i] = slab[2 * channels:3 * channels].astype(BF16)
        g_s[i] = sigmoid(slab[3 * channels:])

    @pl.loop(0, rows // 2)
    def _(pair):
        projections(2 * pair)
        projections(2 * pair + 1)

    for d in range(1, chips):
        bias_copy(chip_core(-d), d, partner).wait_recv()
        relay_copy(chip_core(-d), d).start()
    bias_copy(partner, 0, partner).wait_recv()
    for d in range(1, chips):
        relay_copy(lax.rem(chip - d + chips, chips) * 2 + 1 - core, d).wait_recv()
    for h in range(heads):
        for qh in range(2):
            for kh in range(2):
                keys, queries = slice(kh * LANES, (kh + 1) * LANES), slice(qh * LANES, (qh + 1) * LANES)
                tile = bias_all[h, queries, keys].astype(F32).T if share else bias_all[h, keys, queries].astype(F32)
                logit_bias[h, keys, queries] = (tile + (mask_ref[keys, :] - 1.0) * NEG_BIG) * LOG2E
    scale = width ** -0.5 * LOG2E

    def turn_copy(source, t, p, target, to):
        return pltpu.make_async_remote_copy(
            src_ref=z_nat.at[pl.ds(TURN * t, TURN), pl.ds(pl.multiple_of(to * rows, rows), rows), :], dst_ref=r_buf.at[source, pl.ds(TURN * t, TURN)],
            send_sem=t_send.at[p - 1], recv_sem=t_recv.at[p - 1], device_id={'dap': target}, device_id_type=MESH)

    @pl.loop(0, rows)
    def _(i):
        keys = k_s[i]
        parts = []
        for h in range(heads):
            pieces = [q_s[i, h * width:(h + 1) * width, :]]
            if h:
                pieces = [jnp.zeros((h * width, tokens), BF16)] + pieces
            if h < heads - 1:
                pieces = pieces + [jnp.zeros(((heads - 1 - h) * width, tokens), BF16)]
            scores = dot_nn(keys, jnp.concatenate(pieces, axis=0))
            halves = []
            for qh in range(2):
                lanes = slice(qh * LANES, (qh + 1) * LANES)
                logits = scores[:, lanes] * scale + logit_bias[h, :, lanes]
                weights = jnp.exp2(logits - jnp.max(logits, axis=0, keepdims=True))
                total = jnp.sum(weights, axis=0, keepdims=True)
                halves.append((weights * (1.0 / total)).astype(BF16))
            parts.append(dot_nn(v_s[i, h * width:(h + 1) * width, :], jnp.concatenate(halves, axis=1)))
        merged = (jnp.concatenate(parts, axis=0) * g_s[i]).astype(BF16)
        z_row = (z_ref[i].astype(F32) + dot_nn(w_o[...], merged)).astype(BF16)
        if trans:
            normed = layer_norm_t(z_row)
            hidden = pt_out.shape[1]
            update = jnp.zeros((channels, tokens), F32)
            for part in range(0, hidden, channels):
                first = dot_nn(pt_in_t[part:part + channels, :], normed)
                second = dot_nn(pt_in_t[hidden + part:hidden + part + channels, :], normed)
                update = update + dot_nn(pt_out_t[:, part:part + channels], (first * sigmoid(first) * second).astype(BF16))
            z_row = (z_row.astype(F32) + update).astype(BF16)
        z_nat[i] = turned(z_row)

        if share:
            bias_s[0, pl.ds(pl.multiple_of(i * 8, 8), 8), :], bias_s[1, pl.ds(pl.multiple_of(i * 8, 8), 8), :] = jnp.split(dot_nn(bias_t[layer], layer_norm_t(z_row)), 2, axis=1)

        @pl.when((lax.rem(i, TURN) == 0) & (i > 0))
        def _():
            for p in range(1, n_dev):
                turn_copy(me, i // TURN - 1, p, peers[p - 1], peers[p - 1]).start()

    own = pltpu.make_async_copy(z_nat.at[:, pl.ds(spot, rows), :], r_buf.at[me], own_sem)
    own.start()
    for p in range(1, n_dev):
        turn_copy(me, rows // TURN - 1, p, peers[p - 1], peers[p - 1]).start()
    own.wait()

    def whole(source, p, target):
        return pltpu.make_async_remote_copy(src_ref=r_buf.at[source], dst_ref=r_buf.at[source], send_sem=t_send.at[p - 1], recv_sem=t_recv.at[p - 1], device_id={'dap': target}, device_id_type=MESH)

    def place(source):
        pad = rows + 8
        for i in range(rows):
            stage[i * pad:i * pad + rows, :] = r_buf[source, i].astype(F32)
        for j in range(rows):
            placed_values = stage[pl.ds(j, rows, stride=pad), :].astype(BF16)
            if last:
                out_ref[j, pl.ds(pl.multiple_of(source * rows, rows), rows), :] = placed_values
            else:
                q_all[j, pl.ds(pl.multiple_of(source * rows, rows), rows), :] = placed_values

    q_all = k_s
    place(me)

    @pl.loop(1, n_dev)
    def _(p):
        source = lax.rem(me + n_dev - p, n_dev)
        whole(source, p, lax.rem(me + p, n_dev)).wait_recv()
        place(source)

    if not last:
        @pl.loop(0, rows)
        def _(j):
            out_ref[j] = turned(q_all[j])

    for p in range(1, n_dev):
        whole(me, p, peers[p - 1]).wait_send()
        if share:
            kv_copy(me, p, peers[p - 1]).wait_send()
            kv_copy(lax.rem(me + n_dev - p, n_dev), p, peers[p - 1]).wait_recv()
    for d in range(chips):
        bias_copy(me, d, partner).wait_send()
        if d:
            relay_copy(chip_core(-d), d).wait_send()
    if share:
        for h in range(heads):
            for half in range(2):
                bias_next[h, :, half * LANES:(half + 1) * LANES] = bias_s[half, pl.ds(h, rows, stride=8), :].astype(BF16)


def tri_att(layer, n_dev, cid, last, z, mask, w_qkvg, bias_own, w_out, pt=(), kv=None, bias_t=None):
    rows, channels, tokens = z.shape
    vmem = pl.BlockSpec(memory_space=pltpu.VMEM)
    dma = pltpu.SemaphoreType.DMA
    share = kv is not None
    heads = bias_own.shape[0]
    scratch = [
        pltpu.VMEM((2, rows * 8, LANES), F32),
        pltpu.VMEM((heads, tokens, tokens), BF16),
        pltpu.VMEM((heads, tokens, tokens), F32),
        pltpu.VMEM((4 * channels, channels), BF16),
        pltpu.VMEM((channels, channels), BF16),
        pltpu.VMEM((rows, tokens, channels), BF16),
        pltpu.VMEM((rows, channels, tokens), BF16),
        pltpu.VMEM((rows, channels, tokens), BF16),
        pltpu.VMEM((rows, channels, tokens), F32),
        pltpu.VMEM((rows, tokens, channels), BF16),
        pltpu.VMEM((n_dev, rows, rows, channels), BF16),
        pltpu.VMEM((rows * (rows + 8), LANES), F32),
        dma((n_dev // 2,)), dma((n_dev // 2,)), dma((n_dev // 2,)), dma((n_dev // 2,)), dma((n_dev - 1,)), dma((n_dev - 1,)), dma,
    ]
    if pt:
        scratch += [pltpu.VMEM(pt[0].shape[:0:-1], BF16), pltpu.VMEM(pt[1].shape[:0:-1], BF16)]
    shape = jax.ShapeDtypeStruct((rows, tokens, channels) if last else z.shape, BF16)
    if share:
        kv_shape = jax.ShapeDtypeStruct((tokens, kv.shape[1]), BF16)
        scratch += [dma((n_dev - 1,)), dma((n_dev - 1,))]
        bias_shape = jax.ShapeDtypeStruct(bias_own.shape, BF16)
    return pl.pallas_call(
        functools.partial(tri_att_kernel, layer, n_dev, heads, last, bool(pt), share),
        out_shape=(shape, kv_shape, bias_shape) if share else shape,
        in_specs=[vmem] * (5 + len(pt) + 2 * share),
        out_specs=(vmem, vmem, vmem) if share else vmem,
        scratch_shapes=scratch,
        compiler_params=pltpu.CompilerParams(collective_id=cid, has_side_effects=True, vmem_limit_bytes=VMEM_LIMIT),
        name=f'tri_att_{cid}',
    )(z, mask, w_qkvg, bias_own, w_out, *pt, *((kv, bias_t) if share else ()))


def transition(act_in, w_in, w_out):
    hidden = w_out.shape[0]
    projected = jnp.dot(layer_norm(act_in), w_in, preferred_element_type=F32)
    inner = (jax.nn.silu(projected[..., :hidden]) * projected[..., hidden:]).astype(BF16)
    return (act_in.astype(F32) + jnp.dot(inner, w_out, preferred_element_type=F32)).astype(BF16)


def single_inputs(single, w_qkvg):
    width = w_qkvg.shape[1] // 4
    projected = jnp.dot(layer_norm(single), w_qkvg, preferred_element_type=F32)
    return projected[:, :width].astype(BF16), projected[:, width:3 * width].astype(BF16), jax.nn.sigmoid(projected[:, 3 * width:])


def single_step(single, query, gate, kv_all, pair_bias, mask_all, w_out, st_in, st_out):
    rows, tokens = single.shape[0], kv_all.shape[0]
    heads = pair_bias.shape[1]
    head_dim = query.shape[1] // heads
    query, gate = query.reshape(rows, heads, head_dim), gate.reshape(rows, heads, head_dim)
    kv_all = kv_all.reshape(tokens, 2, heads, head_dim)
    logits = jnp.einsum('ihd,jhd->ihj', query, kv_all[:, 0], preferred_element_type=F32) * head_dim ** -0.5 + pair_bias.astype(F32) + (mask_all - 1.0) * NEG_BIG
    soft_scores = jax.nn.softmax(logits, axis=-1).astype(BF16)
    attended = jnp.einsum('ihj,jhd->ihd', soft_scores, kv_all[:, 1], preferred_element_type=F32)
    merged = (attended * gate).astype(BF16).reshape(rows, -1)
    single = (single.astype(F32) + jnp.dot(merged, w_out, preferred_element_type=F32)).astype(BF16)
    return transition(single, st_in, st_out)


def solution(mesh):
    row_spec = P(('req', 'dap'))
    single_spec = P(('req', 'dap'), None)
    pair_spec = P(('req', 'dap'), None, None)
    n_dev = mesh.shape['dap']

    def local_program(single, pair, token_mask, *weights):
        w = dict(zip(WEIGHT_NAMES, weights))
        blocks = weights[0].shape[0]
        mask = jnp.broadcast_to(token_mask.astype(F32)[:, None], (token_mask.shape[0], LANES))
        heads = w['tas_bias'].shape[2]

        def bias_rows(name):
            swapped = jnp.swapaxes(w[name], 1, 2)
            return jnp.pad(swapped, ((0, 0), (0, 8 - heads), (0, 0)))

        tas_bias, tae_bias = bias_rows('tas_bias'), bias_rows('tae_bias')
        pair = jnp.swapaxes(pair, 1, 2)
        for b in range(blocks):
            cid = 4 * b
            last = b == blocks - 1
            query, kv, gate = single_inputs(single, w['ap_qkvg'][b])
            out = ('row', b, n_dev, cid, b == 0, pair, mask, w['tmo_proj'], w['tmo_gate'], w['tmo_out'])
            if b == 0:
                pair, mask = tri_mult(*out)
            else:
                pair, = tri_mult(*out)
            pair, bias = tri_mult('col', b, n_dev, cid + 1, False, pair, mask, w['tmi_proj'], w['tmi_gate'], w['tmi_out'], tas_bias, heads)
            pair, kv_all, bias = tri_att(b, n_dev, cid + 2, False, pair, mask, w['tas_qkvg'], bias, w['tas_out'], (), kv, tae_bias)
            pair = tri_att(b, n_dev, cid + 3, last, pair, mask, w['tae_qkvg'], bias, w['tae_out'], (w['pt_in'], w['pt_out']))
            if last:
                pair_bias = jnp.einsum('ijc,ch->ihj', layer_norm(pair), w['ap_bias'][b], preferred_element_type=F32).astype(BF16)
            else:
                centred = pair.astype(F32) - jnp.mean(pair.astype(F32), axis=1, keepdims=True)
                normed = (centred * lax.rsqrt(jnp.mean(centred * centred, axis=1, keepdims=True) + EPS)).astype(BF16)
                pair_bias = jnp.einsum('icj,ch->ihj', normed, w['ap_bias'][b], preferred_element_type=F32).astype(BF16)
            single = single_step(single, query, gate, kv_all, pair_bias, mask[:, 0], w['ap_out'][b], w['st_in'][b], w['st_out'][b])
        return single, pair

    return jax.shard_map(local_program, mesh=mesh, in_specs=(single_spec, pair_spec, row_spec) + (P(),) * len(WEIGHT_NAMES), out_specs=(single_spec, pair_spec), check_vma=False)
```

```python
import functools

import jax
import jax.numpy as jnp
from jax import lax
from jax.experimental import pallas as pl
from jax.experimental.pallas import tpu as pltpu
from jax.sharding import PartitionSpec as P

EPS = 1e-5
NEG_BIG = 1e9
LOG2E = 1.4426950408889634
F32 = jnp.float32
BF16 = jnp.bfloat16
MESH = pl.DeviceIdType.MESH
WEIGHT_NAMES = ('tmo_proj', 'tmo_gate', 'tmo_out', 'tmi_proj', 'tmi_gate', 'tmi_out', 'tas_qkvg', 'tas_bias', 'tas_out', 'tae_qkvg', 'tae_bias', 'tae_out', 'pt_in', 'pt_out', 'ap_qkvg', 'ap_bias', 'ap_out', 'st_in', 'st_out')
LANES = 128
TURN = 2
VMEM_LIMIT = 60 * 1024 * 1024


def dot_nn(lhs, rhs):
    return lax.dot_general(lhs, rhs, (((1,), (0,)), ((), ())), preferred_element_type=F32)


def turned(values):
    return values.astype(F32).T.astype(BF16)


def dot_nt(lhs, rhs):
    return lax.dot_general(lhs, rhs, (((1,), (1,)), ((), ())), preferred_element_type=F32)


def dot_tn(lhs, rhs):
    return lax.dot_general(lhs, rhs, (((0,), (0,)), ((), ())), preferred_element_type=F32)


def sigmoid(values):
    return 0.5 * jnp.tanh(0.5 * values) + 0.5


def layer_norm_t(values):
    values = values.astype(F32)
    centred = values - jnp.mean(values, axis=0, keepdims=True)
    variance = jnp.mean(centred * centred, axis=0, keepdims=True)
    return (centred * lax.rsqrt(variance + EPS)).astype(BF16)


def layer_norm(values):
    values = values.astype(F32)
    centred = values - jnp.mean(values, axis=-1, keepdims=True)
    variance = jnp.mean(centred * centred, axis=-1, keepdims=True)
    return (centred * lax.rsqrt(variance + EPS)).astype(BF16)


def tri_mult_kernel(kind, layer, n_dev, first, heads, z_hbm, mask_ref, w_proj, w_gate, w_out, *rest):
    rest = list(rest)
    bias_t = rest.pop(0) if heads else None
    out_ref = rest.pop(0)
    mask_out = rest.pop(0) if first else None
    bias_out = rest.pop(0) if heads else None
    mask_send, mask_recv = (rest.pop(), rest.pop()) if first else (None, None)
    (zfull, b_full, a_full, a_turn, stage, w_t, w_o, w_g, gate_s, x_buf, x_in, mask_l, in_sem, right_send, right_recv, left_send, left_recv, pair_send, pair_recv, x_send, x_recv) = rest
    chips = n_dev // 2
    rows = zfull.shape[2]
    half_c = b_full.shape[0]
    channels = 2 * half_c
    pad = half_c + 8
    me = lax.axis_index('dap')
    chip, core = me // 2, lax.rem(me, 2)
    partner = chip * 2 + 1 - core
    right = lax.rem(chip + 1, chips) * 2 + core
    left = lax.rem(chip + chips - 1, chips) * 2 + core

    loads = [pltpu.make_async_copy(z_hbm.at[:, :, pl.ds(h * LANES, LANES)], zfull.at[me, h], in_sem.at[h]) for h in range(2)]
    for load in loads:
        load.start()
    barrier = pltpu.get_barrier_semaphore()
    greeted = [lax.rem(me + p, n_dev) for p in range(1, n_dev)] if first else [left, right, partner]
    for peer in greeted:
        pl.semaphore_signal(barrier, inc=1, device_id={'dap': peer}, device_id_type=MESH)
    for load in loads:
        load.wait()
    pl.semaphore_wait(barrier, len(greeted))

    def send(block, half, send_sem, recv_sem, target):
        return pltpu.make_async_remote_copy(src_ref=zfull.at[block, half], dst_ref=zfull.at[block, half], send_sem=send_sem, recv_sem=recv_sem, device_id={'dap': target}, device_id_type=MESH)

    send(me, 0, right_send.at[0], right_recv.at[0], right).start()
    send(me, 1, left_send.at[0], left_recv.at[0], left).start()
    send(me, 1, right_send.at[1], right_recv.at[1], right).start()
    send(me, 0, left_send.at[1], left_recv.at[1], left).start()
    send(me, 0, pair_send.at[0], pair_recv.at[0], partner).start()
    send(me, 1, pair_send.at[1], pair_recv.at[1], partner).start()

    def mask_copy(owner, p, target):
        return pltpu.make_async_remote_copy(src_ref=mask_ref, dst_ref=mask_out.at[pl.ds(pl.multiple_of(owner * rows, rows), rows), :], send_sem=mask_send.at[p - 1], recv_sem=mask_recv.at[p - 1], device_id={'dap': target}, device_id_type=MESH)

    if first:
        for p in range(1, n_dev):
            mask_copy(me, p, greeted[p - 1]).start()
        mask_out[pl.ds(pl.multiple_of(me * rows, rows), rows), :] = mask_ref[...]
    masks = mask_out if first else mask_ref

    x_buf[0, 0, :4 * channels, :] = w_proj[layer].astype(F32).T
    for spot, part in enumerate((2, 3, 0, 1)):
        w_t[spot * half_c:(spot + 1) * half_c, :] = x_buf[0, 0, pl.ds(pl.multiple_of(part * channels + core * half_c, half_c), half_c), :].astype(BF16)

    w_own = w_out[layer, pl.ds(pl.multiple_of(core * half_c, half_c), half_c), :]
    w_other = w_out[layer, pl.ds(pl.multiple_of((1 - core) * half_c, half_c), half_c), :]
    w_o[...] = turned(jnp.concatenate([w_own, w_other], axis=0))
    w_g[...] = turned(w_gate[layer])

    my_half = chip // (chips // 2)
    my_off = pl.multiple_of(lax.rem(chip, chips // 2) * 2 * rows, 2 * rows)

    def project(block, half, operands):
        weights = w_t[:operands * channels, :]

        @pl.loop(0, rows // 2)
        def _(pair):
            normed = jnp.concatenate([layer_norm_t(zfull[block, half, 2 * pair + t]) for t in range(2)], axis=1)
            slab = dot_nn(weights, normed)
            for o in range(operands):
                gated = sigmoid(slab[o * channels + half_c:(o + 1) * channels]) * slab[o * channels:o * channels + half_c]
                for t in range(2):
                    row = 2 * pair + t
                    stage[o, pl.ds(pl.multiple_of(row * pad, 8), half_c), :] = gated[:, t * LANES:(t + 1) * LANES]

        spot = pl.multiple_of(block * rows, rows)

        @pl.loop(0, half_c // 16)
        def _(group):
            for t in range(16):
                c = group * 16 + t
                b_full[c, half, pl.ds(spot, rows), :] = stage[0, pl.ds(c, rows, stride=pad), :].astype(BF16)
                if operands == 2:
                    left_operand = stage[1, pl.ds(c, rows, stride=pad), :].astype(BF16)
                    if kind == 'row':
                        a_full[c, half, pl.ds(pl.multiple_of(lax.rem(block, 2) * rows, rows), rows), :] = left_operand
                    else:
                        a_full[c, pl.ds(spot, rows), :] = left_operand

    def process(block, half, mine):
        if kind == 'row':
            project(block, half, 2 if mine else 1)
        else:
            @pl.when(half == my_half)
            def _():
                project(block, half, 2)

            @pl.when(half != my_half)
            def _():
                project(block, half, 1)

    @pl.loop(0, 4)
    def _(t):
        who, half = t // 2, lax.rem(t, 2)
        block = jnp.where(who == 0, me, partner)

        @pl.when(who == 1)
        def _():
            send(partner, half, pair_send.at[half], pair_recv.at[half], partner).wait_recv()

        process(block, half, True)

    events = chips - 1

    def turn_left():
        key_mask = jnp.concatenate([mask_l[0, :1, :], mask_l[1, :1, :]], axis=1).astype(BF16)

        @pl.loop(0, half_c // 4)
        def _(group):
            for t in range(4):
                c = group * 4 + t
                left_operand = jnp.concatenate([a_full[c, 0], a_full[c, 1]], axis=1) if kind == 'row' else a_full[c].T
                a_turn[c] = left_operand * key_mask

    @pl.loop(0, events)
    def _(e):
        dist = e // 2 + 1
        half_r = lax.rem(e, 2)
        half_l = 1 - half_r
        from_left = lax.rem(chip - dist + chips, chips)
        from_right = lax.rem(chip + dist, chips)
        block_r, block_l = from_left * 2 + core, from_right * 2 + core
        send(block_r, half_r, right_send.at[e], right_recv.at[e], right).wait_recv()

        @pl.when(e + 2 < events)
        def _():
            send(block_r, half_r, right_send.at[e + 2], right_recv.at[e + 2], right).start()

        send(block_r, half_r, pair_send.at[2 * e + 2], pair_recv.at[2 * e + 2], partner).start()
        send(block_l, half_l, left_send.at[e], left_recv.at[e], left).wait_recv()

        @pl.when(e + 2 < events)
        def _():
            send(block_l, half_l, left_send.at[e + 2], left_recv.at[e + 2], left).start()

        send(block_l, half_l, pair_send.at[2 * e + 3], pair_recv.at[2 * e + 3], partner).start()

        @pl.when(e == 0)
        def _():
            @pl.loop(0, rows)
            def _(i):
                for half in range(2):
                    gate_s[half, i] = sigmoid(dot_nn(w_g[...], layer_norm_t(zfull[me, half, i])))

        @pl.when(e == 1)
        def _():
            if first:
                for p in range(1, n_dev):
                    mask_copy(lax.rem(me + n_dev - p, n_dev), p, greeted[p - 1]).wait_recv()
            for half in range(2):
                mask_l[half] = masks[half * LANES:(half + 1) * LANES, :].T[:8, :]
            if kind == 'row':
                turn_left()

        @pl.loop(0, 4)
        def _(t):
            side, other = lax.rem(t, 2), t // 2
            owner = jnp.where(other == 0, core, 1 - core)
            block = jnp.where(side == 0, from_left, from_right) * 2 + owner
            half = jnp.where(side == 0, half_r, half_l)

            @pl.when(other == 1)
            def _():
                send(block, half, pair_send.at[2 * e + 2 + side], pair_recv.at[2 * e + 2 + side], partner).wait_recv()

            process(block, half, False)

    if kind != 'row':
        turn_left()

    def exchange(half):
        return pltpu.make_async_remote_copy(src_ref=x_buf.at[1 - core, half], dst_ref=x_in.at[half], send_sem=x_send.at[half], recv_sem=x_recv.at[half], device_id={'dap': partner}, device_id_type=MESH)

    @pl.loop(0, half_c // 4)
    def _(group):
        for t in range(4):
            c = group * 4 + t
            rhs = jnp.concatenate([b_full[c, 0], b_full[c, 1]], axis=1)
            product = dot_nt(a_turn[c], rhs) if kind == 'row' else dot_nn(a_turn[c, pl.ds(my_off, 2 * rows), :], rhs)
            for who in range(2):
                for half in range(2):
                    x_buf[who, half, pl.ds(c, rows, stride=pad), :] = product[who * rows:(who + 1) * rows, half * LANES:(half + 1) * LANES]

    for e in range(events):
        send(me, 0, right_send.at[e], right_recv.at[e], right).wait_send()
        send(me, 0, left_send.at[e], left_recv.at[e], left).wait_send()
    for half in range(2):
        exchange(half).start()
    for half in range(2):
        exchange(half).wait_recv()

        @pl.loop(0, rows // 2)
        def _(pair):
            lanes = slice(half * LANES, (half + 1) * LANES)
            for t in range(2):
                i = 2 * pair + t
                spot = pl.ds(pl.multiple_of(i * pad, 8), half_c)
                x_mask = mask_l[half, :1, :] * masks[pl.ds(me * rows + i, 1), :]
                x = jnp.concatenate([x_buf[core, half, spot, :], x_in[half, spot, :]], axis=0) * x_mask
                update = dot_nn(w_o[...], layer_norm_t(x))
                z_new = (zfull[me, half, i].astype(F32) + gate_s[half, i] * update).astype(BF16)
                out_ref[i, :, lanes] = z_new
                if heads:
                    stage[0, pl.ds(pl.multiple_of((half * rows + i) * 8, 8), 8), :] = dot_nn(bias_t[layer], layer_norm_t(z_new))

    if heads:
        for half in range(2):
            for h in range(heads):
                bias_out[h, :, half * LANES:(half + 1) * LANES] = stage[0, pl.ds(half * rows * 8 + h, rows, stride=8), :].astype(BF16)
    for e in range(2 * events + 2):
        send(me, 0, pair_send.at[e], pair_recv.at[e], partner).wait_send()
    for half in range(2):
        exchange(half).wait_send()
    if first:
        for p in range(1, n_dev):
            mask_copy(me, p, greeted[p - 1]).wait_send()


def tri_mult(kind, layer, n_dev, cid, first, z, mask, w_proj, w_gate, w_out, bias_t=None, heads=0):
    rows, channels, tokens = z.shape
    assert tokens == 2 * LANES and channels == LANES and rows * n_dev == tokens
    half_c = channels // 2
    pad = half_c + 8
    events = n_dev // 2 - 1
    vmem = pl.BlockSpec(memory_space=pltpu.VMEM)
    dma = pltpu.SemaphoreType.DMA
    left_operand = [pltpu.VMEM((half_c, 2, 2 * rows, LANES), BF16), pltpu.VMEM((half_c, 2 * rows, tokens), BF16)]
    shapes = [jax.ShapeDtypeStruct(z.shape, BF16)]
    if first:
        shapes.append(jax.ShapeDtypeStruct((tokens, LANES), F32))
    if heads:
        shapes.append(jax.ShapeDtypeStruct((heads, rows, tokens), BF16))
    if kind != 'row':
        left_operand = [pltpu.VMEM((half_c, tokens, LANES), BF16), pltpu.VMEM((half_c, LANES, tokens), BF16)]
    return pl.pallas_call(
        functools.partial(tri_mult_kernel, kind, layer, n_dev, first, heads),
        out_shape=shapes,
        in_specs=[pl.BlockSpec(memory_space=pl.ANY)] + [vmem] * (4 + bool(heads)),
        out_specs=[vmem] * len(shapes),
        scratch_shapes=[
            pltpu.VMEM((n_dev, 2, rows, channels, LANES), BF16),
            pltpu.VMEM((half_c, 2, tokens, LANES), BF16),
            *left_operand,
            pltpu.VMEM((2, rows * pad, LANES), F32),
            pltpu.VMEM((2 * channels, channels), BF16),
            pltpu.VMEM((channels, channels), BF16),
            pltpu.VMEM((channels, channels), BF16),
            pltpu.VMEM((2, rows, channels, LANES), F32),
            pltpu.VMEM((2, 2, rows * pad, LANES), F32),
            pltpu.VMEM((2, rows * pad, LANES), F32),
            pltpu.VMEM((2, 8, LANES), F32),
            dma((2,)), dma((events,)), dma((events,)), dma((events,)), dma((events,)), dma((2 * events + 2,)), dma((2 * events + 2,)), dma((2,)), dma((2,)),
        ] + [dma((n_dev - 1,)), dma((n_dev - 1,))] * first,
        compiler_params=pltpu.CompilerParams(collective_id=cid, has_side_effects=True, vmem_limit_bytes=VMEM_LIMIT),
        name=f'tri_mult_{kind}_{cid}',
    )(z, mask, w_proj, w_gate, w_out, *((bias_t,) if heads else ()))


def tri_att_kernel(layer, n_dev, heads, last, trans, share, z_ref, mask_ref, w_qkvg, bias_own, w_out, *rest):
    rest = list(rest)
    pt_in, pt_out = (rest.pop(0), rest.pop(0)) if trans else (None, None)
    kv_in, bias_t = (rest.pop(0), rest.pop(0)) if share else (None, None)
    out_ref = rest.pop(0)
    kv_all, bias_next = (rest.pop(0), rest.pop(0)) if share else (None, None)
    (bias_s, bias_all, logit_bias, w_t, w_o, k_s, q_s, v_s, g_s, z_nat, r_buf, stage, b_send, b_recv, d_send, d_recv, t_send, t_recv, own_sem) = rest[:19]
    rest = rest[19:]
    pt_in_t, pt_out_t = (rest.pop(0), rest.pop(0)) if trans else (None, None)
    kv_send, kv_recv = (rest.pop(0), rest.pop(0)) if share else (None, None)
    rows, channels, tokens = z_ref.shape
    width = channels // heads
    me = lax.axis_index('dap')
    barrier = pltpu.get_barrier_semaphore()
    peers = [lax.rem(me + p, n_dev) for p in range(1, n_dev)]
    for peer in peers:
        pl.semaphore_signal(barrier, inc=1, device_id={'dap': peer}, device_id_type=MESH)

    chips = n_dev // 2
    chip, core = me // 2, lax.rem(me, 2)
    partner = chip * 2 + 1 - core
    spot = pl.multiple_of(me * rows, rows)

    def rows_of(ref, owner, lead):
        block = pl.ds(pl.multiple_of(owner * rows, rows), rows)
        return ref.at[:, block, :] if lead else ref.at[block, :]

    def bias_copy(owner, d, target):
        return pltpu.make_async_remote_copy(src_ref=bias_own, dst_ref=rows_of(bias_all, owner, True), send_sem=b_send.at[d], recv_sem=b_recv.at[d], device_id={'dap': target}, device_id_type=MESH)

    def relay_copy(owner, d):
        ref = rows_of(bias_all, owner, True)
        return pltpu.make_async_remote_copy(src_ref=ref, dst_ref=ref, send_sem=d_send.at[d], recv_sem=d_recv.at[d], device_id={'dap': partner}, device_id_type=MESH)

    def kv_copy(owner, p, target):
        return pltpu.make_async_remote_copy(src_ref=kv_in, dst_ref=rows_of(kv_all, owner, False), send_sem=kv_send.at[p - 1], recv_sem=kv_recv.at[p - 1], device_id={'dap': target}, device_id_type=MESH)

    def chip_core(d):
        return lax.rem(chip + d + chips, chips) * 2 + core

    pl.semaphore_wait(barrier, n_dev - 1)
    for d in range(chips):
        bias_copy(me, d, partner if d == 0 else chip_core(d)).start()
    if share:
        for p in range(1, n_dev):
            kv_copy(me, p, peers[p - 1]).start()
        kv_all[pl.ds(spot, rows), :] = kv_in[...]
    bias_all[:, pl.ds(spot, rows), :] = bias_own[...]
    w_t[...] = turned(w_qkvg[layer])
    w_o[...] = turned(w_out[layer])
    if trans:
        for part in range(0, pt_in_t.shape[0], channels):
            pt_in_t[part:part + channels, :] = turned(pt_in[layer, :, part:part + channels])
        pt_out_t[...] = turned(pt_out[layer])

    def projections(i):
        slab = dot_nn(w_t[...], layer_norm_t(z_ref[i]))
        q_s[i] = slab[:channels].astype(BF16)
        k_s[i] = slab[channels:2 * channels].astype(BF16).T
        v_s[i] = slab[2 * channels:3 * channels].astype(BF16)
        g_s[i] = sigmoid(slab[3 * channels:])

    @pl.loop(0, rows // 2)
    def _(pair):
        projections(2 * pair)
        projections(2 * pair + 1)

    for d in range(1, chips):
        bias_copy(chip_core(-d), d, partner).wait_recv()
        relay_copy(chip_core(-d), d).start()
    bias_copy(partner, 0, partner).wait_recv()
    for d in range(1, chips):
        relay_copy(lax.rem(chip - d + chips, chips) * 2 + 1 - core, d).wait_recv()
    for h in range(heads):
        for qh in range(2):
            for kh in range(2):
                keys, queries = slice(kh * LANES, (kh + 1) * LANES), slice(qh * LANES, (qh + 1) * LANES)
                tile = bias_all[h, queries, keys].astype(F32).T if share else bias_all[h, keys, queries].astype(F32)
                logit_bias[h, keys, queries] = (tile + (mask_ref[keys, :] - 1.0) * NEG_BIG) * LOG2E
    scale = width ** -0.5 * LOG2E

    def turn_copy(source, t, p, target, to):
        return pltpu.make_async_remote_copy(
            src_ref=z_nat.at[pl.ds(TURN * t, TURN), pl.ds(pl.multiple_of(to * rows, rows), rows), :], dst_ref=r_buf.at[source, pl.ds(TURN * t, TURN)],
            send_sem=t_send.at[p - 1], recv_sem=t_recv.at[p - 1], device_id={'dap': target}, device_id_type=MESH)

    def one_row(i):
        keys = k_s[i]
        parts = []
        for h in range(heads):
            pieces = [q_s[i, h * width:(h + 1) * width, :]]
            if h:
                pieces = [jnp.zeros((h * width, tokens), BF16)] + pieces
            if h < heads - 1:
                pieces = pieces + [jnp.zeros(((heads - 1 - h) * width, tokens), BF16)]
            scores = dot_nn(keys, jnp.concatenate(pieces, axis=0))
            halves = []
            for qh in range(2):
                lanes = slice(qh * LANES, (qh + 1) * LANES)
                logits = scores[:, lanes] * scale + logit_bias[h, :, lanes]
                weights = jnp.exp2(logits - jnp.max(logits, axis=0, keepdims=True))
                total = jnp.sum(weights, axis=0, keepdims=True)
                halves.append((weights * (1.0 / total)).astype(BF16))
            parts.append(dot_nn(v_s[i, h * width:(h + 1) * width, :], jnp.concatenate(halves, axis=1)))
        merged = (jnp.concatenate(parts, axis=0) * g_s[i]).astype(BF16)
        z_row = (z_ref[i].astype(F32) + dot_nn(w_o[...], merged)).astype(BF16)
        if trans:
            normed = layer_norm_t(z_row)
            hidden = pt_out.shape[1]
            update = jnp.zeros((channels, tokens), F32)
            for part in range(0, hidden, channels):
                first = dot_nn(pt_in_t[part:part + channels, :], normed)
                second = dot_nn(pt_in_t[hidden + part:hidden + part + channels, :], normed)
                update = update + dot_nn(pt_out_t[:, part:part + channels], (first * sigmoid(first) * second).astype(BF16))
            z_row = (z_row.astype(F32) + update).astype(BF16)
        z_nat[i] = z_row.T

        if share:
            bias_s[0, pl.ds(pl.multiple_of(i * 8, 8), 8), :], bias_s[1, pl.ds(pl.multiple_of(i * 8, 8), 8), :] = jnp.split(dot_nn(bias_t[layer], layer_norm_t(z_row)), 2, axis=1)


    @pl.loop(0, rows // 2)
    def _(step):
        for t in range(2):
            one_row(2 * step + t)
        i = 2 * step + 2 - 1

        @pl.when((lax.rem(i, TURN) == TURN - 1) & (i > TURN))
        def _():
            for p in range(1, n_dev):
                turn_copy(me, i // TURN - 1, p, peers[p - 1], peers[p - 1]).start()

    own = pltpu.make_async_copy(z_nat.at[:, pl.ds(spot, rows), :], r_buf.at[me], own_sem)
    own.start()
    for p in range(1, n_dev):
        turn_copy(me, rows // TURN - 1, p, peers[p - 1], peers[p - 1]).start()
    own.wait()

    def whole(source, p, target):
        return pltpu.make_async_remote_copy(src_ref=r_buf.at[source], dst_ref=r_buf.at[source], send_sem=t_send.at[p - 1], recv_sem=t_recv.at[p - 1], device_id={'dap': target}, device_id_type=MESH)

    def place(source):
        pad = rows + 8
        for i in range(rows):
            stage[i * pad:i * pad + rows, :] = r_buf[source, i].astype(F32)
        for j in range(rows):
            placed_values = stage[pl.ds(j, rows, stride=pad), :].astype(BF16)
            if last:
                out_ref[j, pl.ds(pl.multiple_of(source * rows, rows), rows), :] = placed_values
            else:
                q_all[j, pl.ds(pl.multiple_of(source * rows, rows), rows), :] = placed_values

    q_all = k_s
    place(me)

    @pl.loop(1, n_dev)
    def _(p):
        source = lax.rem(me + n_dev - p, n_dev)
        whole(source, p, lax.rem(me + p, n_dev)).wait_recv()
        place(source)

    if not last:
        @pl.loop(0, rows)
        def _(j):
            out_ref[j] = q_all[j].T

    for p in range(1, n_dev):
        whole(me, p, peers[p - 1]).wait_send()
        if share:
            kv_copy(me, p, peers[p - 1]).wait_send()
            kv_copy(lax.rem(me + n_dev - p, n_dev), p, peers[p - 1]).wait_recv()
    for d in range(chips):
        bias_copy(me, d, partner).wait_send()
        if d:
            relay_copy(chip_core(-d), d).wait_send()
    if share:
        for h in range(heads):
            for half in range(2):
                bias_next[h, :, half * LANES:(half + 1) * LANES] = bias_s[half, pl.ds(h, rows, stride=8), :].astype(BF16)


def tri_att(layer, n_dev, cid, last, z, mask, w_qkvg, bias_own, w_out, pt=(), kv=None, bias_t=None):
    rows, channels, tokens = z.shape
    vmem = pl.BlockSpec(memory_space=pltpu.VMEM)
    dma = pltpu.SemaphoreType.DMA
    share = kv is not None
    heads = bias_own.shape[0]
    scratch = [
        pltpu.VMEM((2, rows * 8, LANES), F32),
        pltpu.VMEM((heads, tokens, tokens), BF16),
        pltpu.VMEM((heads, tokens, tokens), F32),
        pltpu.VMEM((4 * channels, channels), BF16),
        pltpu.VMEM((channels, channels), BF16),
        pltpu.VMEM((rows, tokens, channels), BF16),
        pltpu.VMEM((rows, channels, tokens), BF16),
        pltpu.VMEM((rows, channels, tokens), BF16),
        pltpu.VMEM((rows, channels, tokens), F32),
        pltpu.VMEM((rows, tokens, channels), BF16),
        pltpu.VMEM((n_dev, rows, rows, channels), BF16),
        pltpu.VMEM((rows * (rows + 8), LANES), F32),
        dma((n_dev // 2,)), dma((n_dev // 2,)), dma((n_dev // 2,)), dma((n_dev // 2,)), dma((n_dev - 1,)), dma((n_dev - 1,)), dma,
    ]
    if pt:
        scratch += [pltpu.VMEM(pt[0].shape[:0:-1], BF16), pltpu.VMEM(pt[1].shape[:0:-1], BF16)]
    shape = jax.ShapeDtypeStruct((rows, tokens, channels) if last else z.shape, BF16)
    if share:
        kv_shape = jax.ShapeDtypeStruct((tokens, kv.shape[1]), BF16)
        scratch += [dma((n_dev - 1,)), dma((n_dev - 1,))]
        bias_shape = jax.ShapeDtypeStruct(bias_own.shape, BF16)
    return pl.pallas_call(
        functools.partial(tri_att_kernel, layer, n_dev, heads, last, bool(pt), share),
        out_shape=(shape, kv_shape, bias_shape) if share else shape,
        in_specs=[vmem] * (5 + len(pt) + 2 * share),
        out_specs=(vmem, vmem, vmem) if share else vmem,
        scratch_shapes=scratch,
        compiler_params=pltpu.CompilerParams(collective_id=cid, has_side_effects=True, vmem_limit_bytes=VMEM_LIMIT),
        name=f'tri_att_{cid}',
    )(z, mask, w_qkvg, bias_own, w_out, *pt, *((kv, bias_t) if share else ()))


def single_inputs(single, w_qkvg):
    width = w_qkvg.shape[1] // 4
    projected = jnp.dot(layer_norm(single), w_qkvg, preferred_element_type=F32)
    return projected[:, :width].astype(BF16), projected[:, width:3 * width].astype(BF16), jax.nn.sigmoid(projected[:, 3 * width:])


def single_kernel(layer, natural, z_ref, s_ref, q_ref, gate_ref, kv_ref, mask_ref, bias_t, w_out, w_in, w_back, out_ref, bias_s, q_s, o_s, merged_s):
    heads = bias_t.shape[1]
    rows, width = q_ref.shape
    head_dim = width // heads
    lane = lax.broadcasted_iota(jnp.int32, (heads, width), 1)
    head = lax.broadcasted_iota(jnp.int32, (heads, width), 0)
    own_head = ((lane >= head * head_dim) & (lane < (head + 1) * head_dim)).astype(F32)

    @pl.loop(0, rows // 2)
    def _(pair):
        for t in range(2):
            i = 2 * pair + t
            spot = pl.ds(pl.multiple_of(i * heads, heads), heads)
            slab = dot_nt(bias_t[layer], layer_norm(z_ref[i])) if natural else dot_nn(bias_t[layer], layer_norm_t(z_ref[i]))
            bias_s[spot, :] = slab.astype(BF16)
            q_s[spot, :] = (q_ref[pl.ds(i, 1), :] * own_head).astype(BF16)

    key_bias = (jnp.concatenate([mask_ref[half * LANES:(half + 1) * LANES, :].T[:1, :] for half in range(2)], axis=1) - 1.0) * NEG_BIG
    logits = dot_nt(q_s[...], kv_ref[:, :width]) * head_dim ** -0.5 + bias_s[...].astype(F32) + key_bias
    weights = jnp.exp(logits - jnp.max(logits, axis=1, keepdims=True))
    soft = (weights * (1.0 / jnp.sum(weights, axis=1, keepdims=True))).astype(BF16)
    o_s[...] = dot_nn(soft, kv_ref[:, width:])

    @pl.loop(0, rows)
    def _(i):
        merged_s[pl.ds(i, 1), :] = jnp.sum(o_s[pl.ds(pl.multiple_of(i * heads, heads), heads), :] * own_head, axis=0, keepdims=True)

    merged = (merged_s[...] * gate_ref[...]).astype(BF16)
    single = (s_ref[...].astype(F32) + dot_nn(merged, w_out[layer])).astype(BF16)
    normed = layer_norm(single)
    hidden = w_back.shape[1]
    update = jnp.zeros(single.shape, F32)
    part = hidden // 3
    for lo in range(0, hidden, part):
        first = dot_nn(normed, w_in[layer, :, lo:lo + part])
        second = dot_nn(normed, w_in[layer, :, hidden + lo:hidden + lo + part])
        update = update + dot_nn((first * sigmoid(first) * second).astype(BF16), w_back[layer, lo:lo + part, :])
    out_ref[...] = (single.astype(F32) + update).astype(BF16)


def single_step(layer, natural, single, query, gate, kv_all, pair, mask, bias_t, w_out, st_in, st_out):
    rows, width = query.shape
    heads = bias_t.shape[1]
    vmem = pl.BlockSpec(memory_space=pltpu.VMEM)
    return pl.pallas_call(
        functools.partial(single_kernel, layer, natural),
        out_shape=jax.ShapeDtypeStruct(single.shape, BF16),
        in_specs=[vmem] * 10,
        out_specs=vmem,
        scratch_shapes=[
            pltpu.VMEM((rows * heads, kv_all.shape[0]), BF16),
            pltpu.VMEM((rows * heads, width), BF16),
            pltpu.VMEM((rows * heads, width), F32),
            pltpu.VMEM((rows, width), F32),
        ],
        compiler_params=pltpu.CompilerParams(vmem_limit_bytes=VMEM_LIMIT),
        name=f'single_step_{layer}',
    )(pair, single, query.astype(F32), gate, kv_all, mask, bias_t, w_out, st_in, st_out)


def solution(mesh):
    row_spec = P(('req', 'dap'))
    single_spec = P(('req', 'dap'), None)
    pair_spec = P(('req', 'dap'), None, None)
    n_dev = mesh.shape['dap']

    def local_program(single, pair, token_mask, *weights):
        w = dict(zip(WEIGHT_NAMES, weights))
        blocks = weights[0].shape[0]
        mask = jnp.broadcast_to(token_mask.astype(F32)[:, None], (token_mask.shape[0], LANES))
        heads = w['tas_bias'].shape[2]

        def bias_rows(name):
            swapped = jnp.swapaxes(w[name], 1, 2)
            return jnp.pad(swapped, ((0, 0), (0, 8 - heads), (0, 0)))

        tas_bias, tae_bias = bias_rows('tas_bias'), bias_rows('tae_bias')
        ap_bias = jnp.swapaxes(w['ap_bias'], 1, 2)
        pair = jnp.swapaxes(pair, 1, 2)
        for b in range(blocks):
            cid = 4 * b
            last = b == blocks - 1
            query, kv, gate = single_inputs(single, w['ap_qkvg'][b])
            out = ('row', b, n_dev, cid, b == 0, pair, mask, w['tmo_proj'], w['tmo_gate'], w['tmo_out'])
            if b == 0:
                pair, mask = tri_mult(*out)
            else:
                pair, = tri_mult(*out)
            pair, bias = tri_mult('col', b, n_dev, cid + 1, False, pair, mask, w['tmi_proj'], w['tmi_gate'], w['tmi_out'], tas_bias, heads)
            pair, kv_all, bias = tri_att(b, n_dev, cid + 2, False, pair, mask, w['tas_qkvg'], bias, w['tas_out'], (), kv, tae_bias)
            pair = tri_att(b, n_dev, cid + 3, last, pair, mask, w['tae_qkvg'], bias, w['tae_out'], (w['pt_in'], w['pt_out']))
            single = single_step(b, last, single, query, gate, kv_all, pair, mask, ap_bias, w['ap_out'], w['st_in'], w['st_out'])
        return single, pair

    return jax.shard_map(local_program, mesh=mesh, in_specs=(single_spec, pair_spec, row_spec) + (P(),) * len(WEIGHT_NAMES), out_specs=(single_spec, pair_spec), check_vma=False)
```

```python
import functools

import jax
import jax.numpy as jnp
from jax import lax
from jax.experimental import pallas as pl
from jax.experimental.pallas import tpu as pltpu
from jax.sharding import PartitionSpec as P

EPS = 1e-5
NEG_BIG = 1e9
LOG2E = 1.4426950408889634
F32 = jnp.float32
BF16 = jnp.bfloat16
MESH = pl.DeviceIdType.MESH
WEIGHT_NAMES = ('tmo_proj', 'tmo_gate', 'tmo_out', 'tmi_proj', 'tmi_gate', 'tmi_out', 'tas_qkvg', 'tas_bias', 'tas_out', 'tae_qkvg', 'tae_bias', 'tae_out', 'pt_in', 'pt_out', 'ap_qkvg', 'ap_bias', 'ap_out', 'st_in', 'st_out')
LANES = 128
TURN = 2
VMEM_LIMIT = 60 * 1024 * 1024


def dot_nn(lhs, rhs):
    return lax.dot_general(lhs, rhs, (((1,), (0,)), ((), ())), preferred_element_type=F32)


def turned(values):
    return values.astype(F32).T.astype(BF16)


def dot_nt(lhs, rhs):
    return lax.dot_general(lhs, rhs, (((1,), (1,)), ((), ())), preferred_element_type=F32)


def dot_tn(lhs, rhs):
    return lax.dot_general(lhs, rhs, (((0,), (0,)), ((), ())), preferred_element_type=F32)


def bias_rows(w_bias):
    size = w_bias.shape[0]
    eye = lax.broadcasted_iota(jnp.int32, (size, size), 0) == lax.broadcasted_iota(jnp.int32, (size, size), 1)
    return dot_tn(w_bias, eye.astype(F32).astype(BF16)).astype(BF16)


def sigmoid(values):
    return 0.5 * jnp.tanh(0.5 * values) + 0.5


def layer_norm_t(values):
    values = values.astype(F32)
    centred = values - jnp.mean(values, axis=0, keepdims=True)
    variance = jnp.mean(centred * centred, axis=0, keepdims=True)
    return (centred * lax.rsqrt(variance + EPS)).astype(BF16)


def layer_norm(values):
    values = values.astype(F32)
    centred = values - jnp.mean(values, axis=-1, keepdims=True)
    variance = jnp.mean(centred * centred, axis=-1, keepdims=True)
    return (centred * lax.rsqrt(variance + EPS)).astype(BF16)


def tri_mult_kernel(kind, layer, n_dev, first, heads, z_hbm, mask_ref, w_proj, w_gate, w_out, *rest):
    rest = list(rest)
    bias_t = rest.pop(0) if heads else None
    out_ref = rest.pop(0)
    mask_out = rest.pop(0) if first else None
    bias_out = rest.pop(0) if heads else None
    mask_send, mask_recv = (rest.pop(), rest.pop()) if first else (None, None)
    (zfull, b_full, a_full, a_turn, stage, w_t, w_o, w_g, gate_s, x_buf, x_in, mask_l, in_sem, right_send, right_recv, left_send, left_recv, pair_send, pair_recv, x_send, x_recv) = rest
    chips = n_dev // 2
    rows = zfull.shape[2]
    half_c = b_full.shape[0]
    channels = 2 * half_c
    pad = half_c + 8
    me = lax.axis_index('dap')
    chip, core = me // 2, lax.rem(me, 2)
    partner = chip * 2 + 1 - core
    right = lax.rem(chip + 1, chips) * 2 + core
    left = lax.rem(chip + chips - 1, chips) * 2 + core

    loads = [pltpu.make_async_copy(z_hbm.at[:, :, pl.ds(h * LANES, LANES)], zfull.at[me, h], in_sem.at[h]) for h in range(2)]
    for load in loads:
        load.start()
    barrier = pltpu.get_barrier_semaphore()
    greeted = [lax.rem(me + p, n_dev) for p in range(1, n_dev)] if first else [left, right, partner]
    for peer in greeted:
        pl.semaphore_signal(barrier, inc=1, device_id={'dap': peer}, device_id_type=MESH)
    for load in loads:
        load.wait()
    pl.semaphore_wait(barrier, len(greeted))

    def send(block, half, send_sem, recv_sem, target):
        return pltpu.make_async_remote_copy(src_ref=zfull.at[block, half], dst_ref=zfull.at[block, half], send_sem=send_sem, recv_sem=recv_sem, device_id={'dap': target}, device_id_type=MESH)

    send(me, 0, right_send.at[0], right_recv.at[0], right).start()
    send(me, 1, left_send.at[0], left_recv.at[0], left).start()
    send(me, 1, right_send.at[1], right_recv.at[1], right).start()
    send(me, 0, left_send.at[1], left_recv.at[1], left).start()
    send(me, 0, pair_send.at[0], pair_recv.at[0], partner).start()
    send(me, 1, pair_send.at[1], pair_recv.at[1], partner).start()

    def mask_copy(owner, p, target):
        return pltpu.make_async_remote_copy(src_ref=mask_ref, dst_ref=mask_out.at[pl.ds(pl.multiple_of(owner * rows, rows), rows), :], send_sem=mask_send.at[p - 1], recv_sem=mask_recv.at[p - 1], device_id={'dap': target}, device_id_type=MESH)

    if first:
        for p in range(1, n_dev):
            mask_copy(me, p, greeted[p - 1]).start()
        mask_out[pl.ds(pl.multiple_of(me * rows, rows), rows), :] = mask_ref[...]
    masks = mask_out if first else mask_ref

    x_buf[0, 0, :4 * channels, :] = w_proj[layer].astype(F32).T
    for spot, part in enumerate((2, 3, 0, 1)):
        w_t[spot * half_c:(spot + 1) * half_c, :] = x_buf[0, 0, pl.ds(pl.multiple_of(part * channels + core * half_c, half_c), half_c), :].astype(BF16)

    w_own = w_out[layer, pl.ds(pl.multiple_of(core * half_c, half_c), half_c), :]
    w_other = w_out[layer, pl.ds(pl.multiple_of((1 - core) * half_c, half_c), half_c), :]
    w_o[...] = turned(jnp.concatenate([w_own, w_other], axis=0))
    w_g[...] = turned(w_gate[layer])

    my_half = chip // (chips // 2)
    my_off = pl.multiple_of(lax.rem(chip, chips // 2) * 2 * rows, 2 * rows)

    def project(block, half, operands):
        weights = w_t[:operands * channels, :]

        @pl.loop(0, rows // 2)
        def _(pair):
            normed = jnp.concatenate([layer_norm_t(zfull[block, half, 2 * pair + t]) for t in range(2)], axis=1)
            slab = dot_nn(weights, normed)
            for o in range(operands):
                gated = sigmoid(slab[o * channels + half_c:(o + 1) * channels]) * slab[o * channels:o * channels + half_c]
                for t in range(2):
                    row = 2 * pair + t
                    stage[o, pl.ds(pl.multiple_of(row * pad, 8), half_c), :] = gated[:, t * LANES:(t + 1) * LANES]

        spot = pl.multiple_of(block * rows, rows)

        @pl.loop(0, half_c // 16)
        def _(group):
            for t in range(16):
                c = group * 16 + t
                b_full[c, half, pl.ds(spot, rows), :] = stage[0, pl.ds(c, rows, stride=pad), :].astype(BF16)
                if operands == 2:
                    left_operand = stage[1, pl.ds(c, rows, stride=pad), :].astype(BF16)
                    if kind == 'row':
                        a_full[c, half, pl.ds(pl.multiple_of(lax.rem(block, 2) * rows, rows), rows), :] = left_operand
                    else:
                        a_full[c, pl.ds(spot, rows), :] = left_operand

    def process(block, half, mine):
        if kind == 'row':
            project(block, half, 2 if mine else 1)
        else:
            @pl.when(half == my_half)
            def _():
                project(block, half, 2)

            @pl.when(half != my_half)
            def _():
                project(block, half, 1)

    @pl.loop(0, 4)
    def _(t):
        who, half = t // 2, lax.rem(t, 2)
        block = jnp.where(who == 0, me, partner)

        @pl.when(who == 1)
        def _():
            send(partner, half, pair_send.at[half], pair_recv.at[half], partner).wait_recv()

        process(block, half, True)

    events = chips - 1

    def turn_left():
        key_mask = jnp.concatenate([mask_l[0, :1, :], mask_l[1, :1, :]], axis=1).astype(BF16)

        @pl.loop(0, half_c // 4)
        def _(group):
            for t in range(4):
                c = group * 4 + t
                left_operand = jnp.concatenate([a_full[c, 0], a_full[c, 1]], axis=1) if kind == 'row' else a_full[c].T
                a_turn[c] = left_operand * key_mask

    @pl.loop(0, events)
    def _(e):
        dist = e // 2 + 1
        half_r = lax.rem(e, 2)
        half_l = 1 - half_r
        from_left = lax.rem(chip - dist + chips, chips)
        from_right = lax.rem(chip + dist, chips)
        block_r, block_l = from_left * 2 + core, from_right * 2 + core
        send(block_r, half_r, right_send.at[e], right_recv.at[e], right).wait_recv()

        @pl.when(e + 2 < events)
        def _():
            send(block_r, half_r, right_send.at[e + 2], right_recv.at[e + 2], right).start()

        send(block_r, half_r, pair_send.at[2 * e + 2], pair_recv.at[2 * e + 2], partner).start()
        send(block_l, half_l, left_send.at[e], left_recv.at[e], left).wait_recv()

        @pl.when(e + 2 < events)
        def _():
            send(block_l, half_l, left_send.at[e + 2], left_recv.at[e + 2], left).start()

        send(block_l, half_l, pair_send.at[2 * e + 3], pair_recv.at[2 * e + 3], partner).start()

        @pl.when(e == 0)
        def _():
            @pl.loop(0, rows)
            def _(i):
                for half in range(2):
                    gate_s[half, i] = sigmoid(dot_nn(w_g[...], layer_norm_t(zfull[me, half, i])))

        @pl.when(e == 1)
        def _():
            if first:
                for p in range(1, n_dev):
                    mask_copy(lax.rem(me + n_dev - p, n_dev), p, greeted[p - 1]).wait_recv()
            for half in range(2):
                mask_l[half] = masks[half * LANES:(half + 1) * LANES, :].T[:8, :]
            if kind == 'row':
                turn_left()

        @pl.loop(0, 4)
        def _(t):
            side, other = lax.rem(t, 2), t // 2
            owner = jnp.where(other == 0, core, 1 - core)
            block = jnp.where(side == 0, from_left, from_right) * 2 + owner
            half = jnp.where(side == 0, half_r, half_l)

            @pl.when(other == 1)
            def _():
                send(block, half, pair_send.at[2 * e + 2 + side], pair_recv.at[2 * e + 2 + side], partner).wait_recv()

            process(block, half, False)

    if kind != 'row':
        turn_left()

    def exchange(half):
        return pltpu.make_async_remote_copy(src_ref=x_buf.at[1 - core, half], dst_ref=x_in.at[half], send_sem=x_send.at[half], recv_sem=x_recv.at[half], device_id={'dap': partner}, device_id_type=MESH)

    @pl.loop(0, half_c // 4)
    def _(group):
        for t in range(4):
            c = group * 4 + t
            rhs = jnp.concatenate([b_full[c, 0], b_full[c, 1]], axis=1)
            product = dot_nt(a_turn[c], rhs) if kind == 'row' else dot_nn(a_turn[c, pl.ds(my_off, 2 * rows), :], rhs)
            for who in range(2):
                for half in range(2):
                    x_buf[who, half, pl.ds(c, rows, stride=pad), :] = product[who * rows:(who + 1) * rows, half * LANES:(half + 1) * LANES]

    for e in range(events):
        send(me, 0, right_send.at[e], right_recv.at[e], right).wait_send()
        send(me, 0, left_send.at[e], left_recv.at[e], left).wait_send()
    for half in range(2):
        exchange(half).start()
    bias_w = bias_rows(bias_t[layer]) if heads else None
    for half in range(2):
        exchange(half).wait_recv()

        @pl.loop(0, rows // 2)
        def _(pair):
            lanes = slice(half * LANES, (half + 1) * LANES)
            for t in range(2):
                i = 2 * pair + t
                spot = pl.ds(pl.multiple_of(i * pad, 8), half_c)
                x_mask = mask_l[half, :1, :] * masks[pl.ds(me * rows + i, 1), :]
                x = jnp.concatenate([x_buf[core, half, spot, :], x_in[half, spot, :]], axis=0) * x_mask
                update = dot_nn(w_o[...], layer_norm_t(x))
                z_new = (zfull[me, half, i].astype(F32) + gate_s[half, i] * update).astype(BF16)
                out_ref[i, :, lanes] = z_new
                if heads:
                    stage[0, pl.ds(pl.multiple_of((half * rows + i) * 8, 8), heads), :] = dot_nn(bias_w, layer_norm_t(z_new))

    if heads:
        for half in range(2):
            for h in range(heads):
                bias_out[h, :, half * LANES:(half + 1) * LANES] = stage[0, pl.ds(half * rows * 8 + h, rows, stride=8), :].astype(BF16)
    for e in range(2 * events + 2):
        send(me, 0, pair_send.at[e], pair_recv.at[e], partner).wait_send()
    for half in range(2):
        exchange(half).wait_send()
    if first:
        for p in range(1, n_dev):
            mask_copy(me, p, greeted[p - 1]).wait_send()


def tri_mult(kind, layer, n_dev, cid, first, z, mask, w_proj, w_gate, w_out, bias_t=None, heads=0):
    rows, channels, tokens = z.shape
    assert tokens == 2 * LANES and channels == LANES and rows * n_dev == tokens
    half_c = channels // 2
    pad = half_c + 8
    events = n_dev // 2 - 1
    vmem = pl.BlockSpec(memory_space=pltpu.VMEM)
    dma = pltpu.SemaphoreType.DMA
    left_operand = [pltpu.VMEM((half_c, 2, 2 * rows, LANES), BF16), pltpu.VMEM((half_c, 2 * rows, tokens), BF16)]
    shapes = [jax.ShapeDtypeStruct(z.shape, BF16)]
    if first:
        shapes.append(jax.ShapeDtypeStruct((tokens, LANES), F32))
    if heads:
        shapes.append(jax.ShapeDtypeStruct((heads, rows, tokens), BF16))
    if kind != 'row':
        left_operand = [pltpu.VMEM((half_c, tokens, LANES), BF16), pltpu.VMEM((half_c, LANES, tokens), BF16)]
    return pl.pallas_call(
        functools.partial(tri_mult_kernel, kind, layer, n_dev, first, heads),
        out_shape=shapes,
        in_specs=[pl.BlockSpec(memory_space=pl.ANY)] + [vmem] * (4 + bool(heads)),
        out_specs=[vmem] * len(shapes),
        scratch_shapes=[
            pltpu.VMEM((n_dev, 2, rows, channels, LANES), BF16),
            pltpu.VMEM((half_c, 2, tokens, LANES), BF16),
            *left_operand,
            pltpu.VMEM((2, rows * pad, LANES), F32),
            pltpu.VMEM((2 * channels, channels), BF16),
            pltpu.VMEM((channels, channels), BF16),
            pltpu.VMEM((channels, channels), BF16),
            pltpu.VMEM((2, rows, channels, LANES), F32),
            pltpu.VMEM((2, 2, rows * pad, LANES), F32),
            pltpu.VMEM((2, rows * pad, LANES), F32),
            pltpu.VMEM((2, 8, LANES), F32),
            dma((2,)), dma((events,)), dma((events,)), dma((events,)), dma((events,)), dma((2 * events + 2,)), dma((2 * events + 2,)), dma((2,)), dma((2,)),
        ] + [dma((n_dev - 1,)), dma((n_dev - 1,))] * first,
        compiler_params=pltpu.CompilerParams(collective_id=cid, has_side_effects=True, vmem_limit_bytes=VMEM_LIMIT),
        name=f'tri_mult_{kind}_{cid}',
    )(z, mask, w_proj, w_gate, w_out, *((bias_t,) if heads else ()))


def tri_att_kernel(layer, n_dev, heads, last, trans, share, z_ref, mask_ref, w_qkvg, bias_own, w_out, *rest):
    rest = list(rest)
    pt_in, pt_out = (rest.pop(0), rest.pop(0)) if trans else (None, None)
    kv_in, bias_t = (rest.pop(0), rest.pop(0)) if share else (None, None)
    out_ref = rest.pop(0)
    kv_all, bias_next = (rest.pop(0), rest.pop(0)) if share else (None, None)
    (bias_s, bias_all, logit_bias, w_t, w_o, k_s, q_s, v_s, g_s, z_nat, r_buf, stage, b_send, b_recv, d_send, d_recv, t_send, t_recv, own_sem) = rest[:19]
    rest = rest[19:]
    pt_in_t, pt_out_t = (rest.pop(0), rest.pop(0)) if trans else (None, None)
    kv_send, kv_recv = (rest.pop(0), rest.pop(0)) if share else (None, None)
    rows, channels, tokens = z_ref.shape
    width = channels // heads
    me = lax.axis_index('dap')
    barrier = pltpu.get_barrier_semaphore()
    peers = [lax.rem(me + p, n_dev) for p in range(1, n_dev)]
    for peer in peers:
        pl.semaphore_signal(barrier, inc=1, device_id={'dap': peer}, device_id_type=MESH)

    chips = n_dev // 2
    chip, core = me // 2, lax.rem(me, 2)
    partner = chip * 2 + 1 - core
    spot = pl.multiple_of(me * rows, rows)

    def rows_of(ref, owner, lead):
        block = pl.ds(pl.multiple_of(owner * rows, rows), rows)
        return ref.at[:, block, :] if lead else ref.at[block, :]

    def bias_copy(owner, d, target):
        return pltpu.make_async_remote_copy(src_ref=bias_own, dst_ref=rows_of(bias_all, owner, True), send_sem=b_send.at[d], recv_sem=b_recv.at[d], device_id={'dap': target}, device_id_type=MESH)

    def relay_copy(owner, d):
        ref = rows_of(bias_all, owner, True)
        return pltpu.make_async_remote_copy(src_ref=ref, dst_ref=ref, send_sem=d_send.at[d], recv_sem=d_recv.at[d], device_id={'dap': partner}, device_id_type=MESH)

    def kv_copy(owner, p, target):
        return pltpu.make_async_remote_copy(src_ref=kv_in, dst_ref=rows_of(kv_all, owner, False), send_sem=kv_send.at[p - 1], recv_sem=kv_recv.at[p - 1], device_id={'dap': target}, device_id_type=MESH)

    def chip_core(d):
        return lax.rem(chip + d + chips, chips) * 2 + core

    pl.semaphore_wait(barrier, n_dev - 1)
    for d in range(chips):
        bias_copy(me, d, partner if d == 0 else chip_core(d)).start()
    if share:
        for p in range(1, n_dev):
            kv_copy(me, p, peers[p - 1]).start()
        kv_all[pl.ds(spot, rows), :] = kv_in[...]
    bias_all[:, pl.ds(spot, rows), :] = bias_own[...]
    w_t[...] = turned(w_qkvg[layer])
    w_o[...] = turned(w_out[layer])
    if trans:
        for part in range(0, pt_in_t.shape[0], channels):
            pt_in_t[part:part + channels, :] = turned(pt_in[layer, :, part:part + channels])
        pt_out_t[...] = turned(pt_out[layer])

    def projections(i):
        slab = dot_nn(w_t[...], layer_norm_t(z_ref[i]))
        q_s[i] = slab[:channels].astype(BF16)
        k_s[i] = slab[channels:2 * channels].astype(BF16).T
        v_s[i] = slab[2 * channels:3 * channels].astype(BF16)
        g_s[i] = sigmoid(slab[3 * channels:])

    @pl.loop(0, rows // 2)
    def _(pair):
        projections(2 * pair)
        projections(2 * pair + 1)

    for d in range(1, chips):
        bias_copy(chip_core(-d), d, partner).wait_recv()
        relay_copy(chip_core(-d), d).start()
    bias_copy(partner, 0, partner).wait_recv()
    for d in range(1, chips):
        relay_copy(lax.rem(chip - d + chips, chips) * 2 + 1 - core, d).wait_recv()
    for h in range(heads):
        for qh in range(2):
            for kh in range(2):
                keys, queries = slice(kh * LANES, (kh + 1) * LANES), slice(qh * LANES, (qh + 1) * LANES)
                tile = bias_all[h, queries, keys].astype(F32).T if share else bias_all[h, keys, queries].astype(F32)
                logit_bias[h, keys, queries] = (tile + (mask_ref[keys, :] - 1.0) * NEG_BIG) * LOG2E
    scale = width ** -0.5 * LOG2E

    def turn_copy(source, t, p, target, to):
        return pltpu.make_async_remote_copy(
            src_ref=z_nat.at[pl.ds(TURN * t, TURN), pl.ds(pl.multiple_of(to * rows, rows), rows), :], dst_ref=r_buf.at[source, pl.ds(TURN * t, TURN)],
            send_sem=t_send.at[p - 1], recv_sem=t_recv.at[p - 1], device_id={'dap': target}, device_id_type=MESH)

    bias_w = bias_rows(bias_t[layer]) if share else None

    def one_row(i):
        keys = k_s[i]
        parts = []
        for h in range(heads):
            pieces = [q_s[i, h * width:(h + 1) * width, :]]
            if h:
                pieces = [jnp.zeros((h * width, tokens), BF16)] + pieces
            if h < heads - 1:
                pieces = pieces + [jnp.zeros(((heads - 1 - h) * width, tokens), BF16)]
            scores = dot_nn(keys, jnp.concatenate(pieces, axis=0))
            halves = []
            for qh in range(2):
                lanes = slice(qh * LANES, (qh + 1) * LANES)
                logits = scores[:, lanes] * scale + logit_bias[h, :, lanes]
                weights = jnp.exp2(logits - jnp.max(logits, axis=0, keepdims=True))
                total = jnp.sum(weights, axis=0, keepdims=True)
                halves.append((weights * (1.0 / total)).astype(BF16))
            parts.append(dot_nn(v_s[i, h * width:(h + 1) * width, :], jnp.concatenate(halves, axis=1)))
        merged = (jnp.concatenate(parts, axis=0) * g_s[i]).astype(BF16)
        z_row = (z_ref[i].astype(F32) + dot_nn(w_o[...], merged)).astype(BF16)
        if trans:
            normed = layer_norm_t(z_row)
            hidden = pt_out.shape[1]
            update = jnp.zeros((channels, tokens), F32)
            for part in range(0, hidden, channels):
                first = dot_nn(pt_in_t[part:part + channels, :], normed)
                second = dot_nn(pt_in_t[hidden + part:hidden + part + channels, :], normed)
                update = update + dot_nn(pt_out_t[:, part:part + channels], (first * sigmoid(first) * second).astype(BF16))
            z_row = (z_row.astype(F32) + update).astype(BF16)

        z_nat[i] = z_row.T
        if share:
            slab = dot_nn(bias_w, layer_norm_t(z_row))
            for half in range(2):
                bias_s[half, pl.ds(pl.multiple_of(i * 8, 8), heads), :] = slab[:, half * LANES:(half + 1) * LANES]


    @pl.loop(0, rows // 2)
    def _(step):
        for t in range(2):
            one_row(2 * step + t)
        late = 0 if share else 1

        @pl.when(step >= late)
        def _():
            for p in range(1, n_dev):
                turn_copy(me, step - late, p, peers[p - 1], peers[p - 1]).start()

    own = pltpu.make_async_copy(z_nat.at[:, pl.ds(spot, rows), :], r_buf.at[me], own_sem)
    own.start()
    if not share:
        for p in range(1, n_dev):
            turn_copy(me, rows // TURN - 1, p, peers[p - 1], peers[p - 1]).start()
    own.wait()

    def whole(source, p, target):
        return pltpu.make_async_remote_copy(src_ref=r_buf.at[source], dst_ref=r_buf.at[source], send_sem=t_send.at[p - 1], recv_sem=t_recv.at[p - 1], device_id={'dap': target}, device_id_type=MESH)

    def place(source):
        pad = rows + 8
        for i in range(rows):
            stage[i * pad:i * pad + rows, :] = r_buf[source, i].astype(F32)
        for j in range(rows):
            placed_values = stage[pl.ds(j, rows, stride=pad), :].astype(BF16)
            if last:
                out_ref[j, pl.ds(pl.multiple_of(source * rows, rows), rows), :] = placed_values
            else:
                q_all[j, pl.ds(pl.multiple_of(source * rows, rows), rows), :] = placed_values

    q_all = k_s
    place(me)

    @pl.loop(1, n_dev)
    def _(p):
        source = lax.rem(me + n_dev - p, n_dev)
        whole(source, p, lax.rem(me + p, n_dev)).wait_recv()
        place(source)

    if not last:
        @pl.loop(0, rows // 4)
        def _(group):
            for t in range(4):
                out_ref[group * 4 + t] = q_all[group * 4 + t].T

    for p in range(1, n_dev):
        whole(me, p, peers[p - 1]).wait_send()
        if share:
            kv_copy(me, p, peers[p - 1]).wait_send()
            kv_copy(lax.rem(me + n_dev - p, n_dev), p, peers[p - 1]).wait_recv()
    for d in range(chips):
        bias_copy(me, d, partner).wait_send()
        if d:
            relay_copy(chip_core(-d), d).wait_send()
    if share:
        for h in range(heads):
            for half in range(2):
                bias_next[h, :, half * LANES:(half + 1) * LANES] = bias_s[half, pl.ds(h, rows, stride=8), :].astype(BF16)


def tri_att(layer, n_dev, cid, last, z, mask, w_qkvg, bias_own, w_out, pt=(), kv=None, bias_t=None):
    rows, channels, tokens = z.shape
    vmem = pl.BlockSpec(memory_space=pltpu.VMEM)
    dma = pltpu.SemaphoreType.DMA
    share = kv is not None
    heads = bias_own.shape[0]
    scratch = [
        pltpu.VMEM((2, rows * 8, LANES), F32),
        pltpu.VMEM((heads, tokens, tokens), BF16),
        pltpu.VMEM((heads, tokens, tokens), F32),
        pltpu.VMEM((4 * channels, channels), BF16),
        pltpu.VMEM((channels, channels), BF16),
        pltpu.VMEM((rows, tokens, channels), BF16),
        pltpu.VMEM((rows, channels, tokens), BF16),
        pltpu.VMEM((rows, channels, tokens), BF16),
        pltpu.VMEM((rows, channels, tokens), F32),
        pltpu.VMEM((rows, tokens, channels), BF16),
        pltpu.VMEM((n_dev, rows, rows, channels), BF16),
        pltpu.VMEM((rows * (rows + 8), LANES), F32),
        dma((n_dev // 2,)), dma((n_dev // 2,)), dma((n_dev // 2,)), dma((n_dev // 2,)), dma((n_dev - 1,)), dma((n_dev - 1,)), dma,
    ]
    if pt:
        scratch += [pltpu.VMEM(pt[0].shape[:0:-1], BF16), pltpu.VMEM(pt[1].shape[:0:-1], BF16)]
    shape = jax.ShapeDtypeStruct((rows, tokens, channels) if last else z.shape, BF16)
    if share:
        kv_shape = jax.ShapeDtypeStruct((tokens, kv.shape[1]), BF16)
        scratch += [dma((n_dev - 1,)), dma((n_dev - 1,))]
        bias_shape = jax.ShapeDtypeStruct(bias_own.shape, BF16)
    return pl.pallas_call(
        functools.partial(tri_att_kernel, layer, n_dev, heads, last, bool(pt), share),
        out_shape=(shape, kv_shape, bias_shape) if share else shape,
        in_specs=[vmem] * (5 + len(pt) + 2 * share),
        out_specs=(vmem, vmem, vmem) if share else vmem,
        scratch_shapes=scratch,
        compiler_params=pltpu.CompilerParams(collective_id=cid, has_side_effects=True, vmem_limit_bytes=VMEM_LIMIT),
        name=f'tri_att_{cid}',
    )(z, mask, w_qkvg, bias_own, w_out, *pt, *((kv, bias_t) if share else ()))


def single_kernel(layer, natural, z_ref, s_ref, proj_ref, kv_ref, mask_ref, bias_t, w_out, w_in, w_back, out_ref, bias_s, q_s, o_s, merged_s):
    heads = bias_t.shape[1]
    rows, width = s_ref.shape[0], kv_ref.shape[1] // 2
    head_dim = width // heads
    lane = lax.broadcasted_iota(jnp.int32, (heads, width), 1)
    head = lax.broadcasted_iota(jnp.int32, (heads, width), 0)
    own_head = ((lane >= head * head_dim) & (lane < (head + 1) * head_dim)).astype(F32)

    @pl.loop(0, rows // 2)
    def _(pair):
        for t in range(2):
            i = 2 * pair + t
            spot = pl.ds(pl.multiple_of(i * heads, heads), heads)
            slab = dot_nt(bias_t[layer], layer_norm(z_ref[i])) if natural else dot_nn(bias_t[layer], layer_norm_t(z_ref[i]))
            bias_s[spot, :] = slab.astype(BF16)
            q_s[spot, :] = (proj_ref[pl.ds(i, 1), :width] * own_head).astype(BF16)

    key_bias = (jnp.concatenate([mask_ref[half * LANES:(half + 1) * LANES, :].T[:1, :] for half in range(2)], axis=1) - 1.0) * NEG_BIG
    logits = dot_nt(q_s[...], kv_ref[:, :width]) * head_dim ** -0.5 + bias_s[...].astype(F32) + key_bias
    weights = jnp.exp(logits - jnp.max(logits, axis=1, keepdims=True))
    soft = (weights * (1.0 / jnp.sum(weights, axis=1, keepdims=True))).astype(BF16)
    o_s[...] = dot_nn(soft, kv_ref[:, width:])

    @pl.loop(0, rows)
    def _(i):
        merged_s[pl.ds(i, 1), :] = jnp.sum(o_s[pl.ds(pl.multiple_of(i * heads, heads), heads), :] * own_head, axis=0, keepdims=True)

    merged = (merged_s[...] * sigmoid(proj_ref[:, 3 * width:])).astype(BF16)
    single = (s_ref[...].astype(F32) + dot_nn(merged, w_out[layer])).astype(BF16)
    normed = layer_norm(single)
    hidden = w_back.shape[1]
    update = jnp.zeros(single.shape, F32)
    part = hidden // 3
    for lo in range(0, hidden, part):
        first = dot_nn(normed, w_in[layer, :, lo:lo + part])
        second = dot_nn(normed, w_in[layer, :, hidden + lo:hidden + lo + part])
        update = update + dot_nn((first * sigmoid(first) * second).astype(BF16), w_back[layer, lo:lo + part, :])
    out_ref[...] = (single.astype(F32) + update).astype(BF16)


def single_step(layer, natural, single, projected, kv_all, pair, mask, bias_t, w_out, st_in, st_out):
    rows, width = single.shape[0], kv_all.shape[1] // 2
    heads = bias_t.shape[1]
    vmem = pl.BlockSpec(memory_space=pltpu.VMEM)
    return pl.pallas_call(
        functools.partial(single_kernel, layer, natural),
        out_shape=jax.ShapeDtypeStruct(single.shape, BF16),
        in_specs=[vmem] * 9,
        out_specs=vmem,
        scratch_shapes=[
            pltpu.VMEM((rows * heads, kv_all.shape[0]), BF16),
            pltpu.VMEM((rows * heads, width), BF16),
            pltpu.VMEM((rows * heads, width), F32),
            pltpu.VMEM((rows, width), F32),
        ],
        compiler_params=pltpu.CompilerParams(vmem_limit_bytes=VMEM_LIMIT),
        name=f'single_step_{layer}',
    )(pair, single, projected, kv_all, mask, bias_t, w_out, st_in, st_out)


def solution(mesh):
    row_spec = P(('req', 'dap'))
    single_spec = P(('req', 'dap'), None)
    pair_spec = P(('req', 'dap'), None, None)
    n_dev = mesh.shape['dap']

    def local_program(single, pair, token_mask, *weights):
        w = dict(zip(WEIGHT_NAMES, weights))
        blocks = weights[0].shape[0]
        mask = jnp.broadcast_to(token_mask.astype(F32)[:, None], (token_mask.shape[0], LANES))
        heads = w['tas_bias'].shape[2]

        ap_bias = jnp.swapaxes(w['ap_bias'], 1, 2)
        pair = jnp.swapaxes(pair, 1, 2)
        for b in range(blocks):
            cid = 4 * b
            last = b == blocks - 1
            projected = jnp.dot(layer_norm(single), w['ap_qkvg'][b], preferred_element_type=F32)
            width = projected.shape[1] // 4
            kv = projected[:, width:3 * width].astype(BF16)
            out = ('row', b, n_dev, cid, b == 0, pair, mask, w['tmo_proj'], w['tmo_gate'], w['tmo_out'])
            if b == 0:
                pair, mask = tri_mult(*out)
            else:
                pair, = tri_mult(*out)
            pair, bias = tri_mult('col', b, n_dev, cid + 1, False, pair, mask, w['tmi_proj'], w['tmi_gate'], w['tmi_out'], w['tas_bias'], heads)
            pair, kv_all, bias = tri_att(b, n_dev, cid + 2, False, pair, mask, w['tas_qkvg'], bias, w['tas_out'], (), kv, w['tae_bias'])
            pair = tri_att(b, n_dev, cid + 3, last, pair, mask, w['tae_qkvg'], bias, w['tae_out'], (w['pt_in'], w['pt_out']))
            single = single_step(b, last, single, projected, kv_all, pair, mask, ap_bias, w['ap_out'], w['st_in'], w['st_out'])
        return single, pair

    return jax.shard_map(local_program, mesh=mesh, in_specs=(single_spec, pair_spec, row_spec) + (P(),) * len(WEIGHT_NAMES), out_specs=(single_spec, pair_spec), check_vma=False)
```
